32 devices in a mesh: band: 16 (over z, y, x), ga: 2 (over core).
Axes of the slice: x: 2, y: 2, z: 4, core: 2. Of those that a mesh axis runs over, the one named last changes fastest.
Arguments:
- matrix_elements: float32 [2, 4096, 12288], P(None, 'band', 'ga'), may hold values from -6 to 6
- band_index: int32 [4096], P('band'), may hold values from 0 to 1048575
- occupied: int32 [1], replicated, may hold values from 262144 to 786432
- band_weight: float32 [4096], P('band'), may hold values from 0.3 to 3
- coulomb: float32 [12288], replicated, may hold values from 0.2 to 5
Outputs:
- sigma: float32 [12288, 2, 512], P(('ga', 'band'))
The draws below stay inside these ranges and needn't reach their ends.
All inputs are finite; a program needn't handle non-finite values.
Results may differ from the reference program's by a relative error of at most 0.00018.
Values sent between devices are 32-bit elements; how exact they have to be, the bound alone decides.
A program may use at most 192 MiB of HBM per device.

```python
import math
import jax
import jax.numpy as jnp
from jax import lax

NG = 12288
COLS = 512
NB = 4096


def place_ends(drawn, rng, least, top_value):
    index_at = [jax.random.randint(jax.random.fold_in(rng, axis), (), 0, length) for axis, length in enumerate(drawn.shape)]
    widest = drawn.shape.index(max(drawn.shape))
    neighbour = index_at[:widest] + [(index_at[widest] + 1) % drawn.shape[widest]] + index_at[widest + 1:]
    return drawn.at[tuple(index_at)].set(least).at[tuple(neighbour)].set(top_value)


def strengthened(result, own_key, source, target, blocks, factor):
    owner, partner = [(jnp.arange(result.shape[axis_at]) // (result.shape[axis_at] // blocks)).reshape([-1 if axis == axis_at else 1 for axis in range(result.ndim)]) for axis_at in (source, target)]
    chosen = jax.random.permutation(own_key, blocks)[partner]
    strong = (owner == chosen) | (owner == (partner + blocks // 2) % blocks)
    return jnp.where(strong, factor * result, result)


def shard_levels(stream_key, shape, shards, smallest, top_value):
    level, own = 1.0, jax.random.fold_in(stream_key, 6)
    for axis_at, parts in shards:
        draws = jnp.exp(jax.random.uniform(jax.random.fold_in(own, axis_at), (parts,), jnp.float32, smallest / len(shards), top_value / len(shards)))
        level = level * jnp.repeat(draws, shape[axis_at] // parts).reshape([-1 if axis == axis_at else 1 for axis in range(len(shape))])
    return level


def bell_draw_with(stream_key, shape, width, bound, cuts, heavy, dtype=jnp.bfloat16):
    drawn = width * jax.random.normal(stream_key, shape, jnp.float32)
    if cuts:
        drawn = drawn * shard_levels(stream_key, shape, cuts, -0.22, 0.18)
    return jnp.clip(strengthened(drawn, jax.random.fold_in(stream_key, 3), *heavy), -bound, bound).astype(dtype)


def setup_inputs(seed: int = 0) -> dict:
    arg_keys = jax.random.split(jax.random.key(seed), 6)
    return {
        "matrix_elements": bell_draw_with(arg_keys[0], (2, NB, NG), 1.0, 6.0, ((1, 16), (2, 2)), (1, 2, 16, 2.0), jnp.float32),
        "band_index": place_ends(jax.random.randint(arg_keys[1], (NB,), 0, 1048576), jax.random.fold_in(arg_keys[1], 1), 0, 1048575).astype(jnp.int32),
        "occupied": jax.random.randint(arg_keys[2], (1,), 262144, 786433).astype(jnp.int32),
        "band_weight": jnp.clip(jnp.exp(math.log(3.0) - 2.3025851 * jax.random.uniform(arg_keys[3], (NB,), jnp.float32) ** shard_levels(arg_keys[3], (NB,), ((0, 16),), -0.2, 0.2)), 0.3, 3.0),
        "coulomb": jnp.clip(jnp.exp(jax.random.uniform(arg_keys[4], (NG,), jnp.float32, math.log(0.2), math.log(5.0))), 0.2, 5.0),
    }


def reference(matrix_elements, band_index, occupied, band_weight, coulomb):
    occ = (band_index < occupied[0]).astype(jnp.float32)
    coef = (0.5 - occ) * band_weight
    real = matrix_elements[0]
    imag = matrix_elements[1]
    left = jnp.concatenate([coef[:, None] * real, coef[:, None] * imag], 0)
    slab_re = real[:, :COLS]
    slab_im = imag[:, :COLS]
    right = jnp.concatenate([jnp.concatenate([slab_re, slab_im], 1), jnp.concatenate([slab_im, -slab_re], 1)], 0)
    factor = 1.0 / math.sqrt(NB)
    sums = lax.dot_general(left, right, (((0,), (0,)), ((), ())), precision=lax.Precision.HIGHEST, preferred_element_type=jnp.float32) * factor
    square = 2.0 - real * real - imag * imag
    defect = jnp.dot(coef, square, precision=lax.Precision.HIGHEST, preferred_element_type=jnp.float32) * factor
    weight = jnp.sqrt(coulomb[:, None] * coulomb[None, :COLS])
    part_re = weight * (sums[:, :COLS] + 0.5 * (defect[:, None] + defect[None, :COLS]))
    part_im = weight * sums[:, COLS:]
    return jnp.stack([part_re, part_im], 1)
```

```python
import functools
import math

import jax
import jax.numpy as jnp
from jax import lax
from jax.experimental import pallas as pl
from jax.experimental.pallas import tpu as pltpu
from jax.sharding import PartitionSpec as P

COLS = 512
LANES = 128
CHUNKS = 3
VMEM_BYTES = 67043328

BIT = {"x": 0, "y": 1, "z": 2}
TOP = 3
SLOT = {"x": 1, "y": 2, "z": 3}
ORDERS = {
    (0, 1): "xyz", (0, 0): "yxz", (1, 1): "yxz", (1, 0): "xyz", (2, 1): "zxy", (2, 0): "zyx",
}
DEPTH = 2
STEPS = (
    ("m", 0, 1, 3), ("m", 0, 1, 2), ("m", 1, 1, 3), ("m", 1, 1, 2), ("m", 2, 0, 3), ("m", 2, 0, 2), ("prep", "o"),
    ("slab", "x"), ("slab", "y"), ("m", 2, 0, 1), ("m", 0, 1, 1), ("m", 0, 0, 3), ("m", 2, 0, 0), ("slab", "z"),
    ("m", 0, 1, 0), ("m", 0, 0, 2), ("m", 2, 1, 3), ("fwd", "x"), ("fwd", "y"), ("prep", "x"), ("dot", 0, 1, 1),
    ("s2", 0, 1, 1), ("m", 1, 0, 3), ("prep", "y"), ("dot", 1, 1, 1), ("s2", 1, 1, 1), ("s2", 0, 1, 0),
    ("m", 2, 1, 2), ("dot", 0, 1, 0), ("dot", 0, 0, 1), ("s2", 1, 1, 0), ("fwd", "z"), ("m", 2, 1, 1), ("prep", "z"),
    ("dot", 2, 0, 1), ("a2", 0, 1, 1), ("s3", 0, 1), ("dot", 2, 1, 1), ("m", 1, 1, 1), ("dot", 2, 0, 0),
    ("s2", 2, 1, 1), ("m", 2, 1, 0), ("m", 1, 1, 0), ("a2", 0, 1, 0), ("s2", 2, 1, 0), ("m", 0, 0, 1), ("a3", 0, 1),
    ("s4", 0), ("m", 0, 0, 0), ("dot", 1, 1, 0), ("a2", 1, 1, 1), ("s3", 1, 1), ("a2", 1, 1, 0), ("dot", 2, 1, 0),
    ("a2", 2, 1, 1), ("s2", 0, 0, 1), ("s2", 2, 0, 1), ("s2", 2, 0, 0), ("dot", 0, 0, 0), ("m", 1, 0, 2),
    ("a2", 2, 1, 0), ("s3", 2, 1), ("a2", 2, 0, 1), ("a3", 1, 1), ("s4", 1), ("s2", 0, 0, 0), ("a2", 0, 0, 1),
    ("s3", 0, 0), ("m", 1, 0, 1), ("dot", 1, 0, 1), ("s2", 1, 0, 1), ("a2", 2, 0, 0), ("m", 1, 0, 0),
    ("s2", 1, 0, 0), ("a2", 0, 0, 0), ("a3", 2, 1), ("s4", 2), ("a3", 0, 0), ("a4", 0), ("s3", 2, 0),
    ("dot", 1, 0, 0), ("a2", 1, 0, 1), ("s3", 1, 0), ("a3", 2, 0), ("a2", 1, 0, 0), ("a4", 2), ("a3", 1, 0),
    ("a4", 1),
)


def contract(left, right):
    return lax.dot_general(
        left,
        right,
        (((0,), (0,)), ((), ())),
        precision=lax.Precision.HIGH,
        preferred_element_type=jnp.float32,
    )


def right_side(slab):
    return jnp.concatenate(
        [jnp.concatenate([slab[0], slab[1]], 1), jnp.concatenate([slab[1], -slab[0]], 1)], 0
    )


def defects(coef, block):
    return jnp.sum(coef[:, None] * (2.0 - block[0] * block[0] - block[1] * block[1]), 0)


def body_plain(matrix_elements, band_index, occupied, band_weight, coulomb):
    bands_dev = matrix_elements.shape[1]
    half = matrix_elements.shape[2]
    n_band = lax.axis_size("band")
    n_bits = n_band.bit_length() - 1
    rows_dev = half // n_band
    n_ga = lax.axis_size("ga")
    chunks = 3 if rows_dev % 3 == 0 else 1
    width = rows_dev // chunks
    factor = 1.0 / math.sqrt(bands_dev * n_band)
    band_pos = lax.axis_index("band")
    ga_pos = lax.axis_index("ga")
    bits = list(range(n_bits - 1))
    top = n_band // 2
    firsts = [b % len(bits) for b in range(chunks)]
    streams = [(c, p) for p in range(2) for c in range(chunks)]
    orders = {}
    for c, p in streams:
        rest = bits[firsts[c] + 1 :] + bits[: firsts[c]]
        orders[c, p] = rest[p:] + rest[:p]

    def swap(x, bit):
        return lax.ppermute(x, "band", [(i, i ^ (1 << bit)) for i in range(n_band)])

    def mine(bit):
        return (band_pos >> bit) & 1

    def pick(x, c, p, which):
        bit = firsts[c]
        parts = []
        for d in range(p * top, (p + 1) * top):
            if not (d >> bit) & 1:
                low = d * rows_dev + c * width
                high = (d | (1 << bit)) * rows_dev + c * width
                parts.append(
                    jnp.where(which == 1, x[..., high : high + width], x[..., low : low + width])
                )
        return jnp.concatenate(parts, -1)

    there = {
        (c, p): swap(pick(matrix_elements, c, p, 1 - mine(firsts[c])), firsts[c])
        for c, p in streams
    }

    occ = (band_index < occupied[0]).astype(jnp.float32)
    coef = (0.5 - occ) * band_weight
    first = matrix_elements[:, :, :COLS]
    moved = lax.ppermute(first, "ga", [(0, g) for g in range(1, n_ga)][:1])
    slab = jnp.where(ga_pos == 0, first, moved)
    scaled = coef[None, :, None] * slab
    right = right_side(scaled)
    rights = [right_side(swap(scaled, bit)) for bit in firsts]
    row_def = defects(coef, matrix_elements)
    col_def = defects(coef, slab)

    sums, left = {}, {}
    for c, p in streams:
        bit = firsts[c]
        rows_here = pick(row_def, c, p, mine(bit))
        send = jnp.concatenate([pick(row_def, c, p, 1 - mine(bit)), col_def])
        got = swap(send, bit)
        count = rows_here.shape[0]
        rows_sum = rows_here + got[:count]
        cols_sum = col_def + got[count:]
        here = pick(matrix_elements, c, p, mine(bit))
        part = contract(here.reshape(2 * bands_dev, count), right)
        part = part + contract(there[c, p].reshape(2 * bands_dev, count), rights[c])
        extra = 0.5 * (rows_sum[:, None] + cols_sum[None, :])
        part = part + jnp.concatenate([extra, jnp.zeros_like(extra)], 1)
        sums[c, p] = part.reshape((2,) * (n_bits - 2) + (width, 2 * COLS))
        left[c, p] = [b for b in reversed(bits) if b != bit]

    for step in range(n_bits - 2):
        sent = {}
        for k in streams:
            bit = orders[k][step]
            send = lax.dynamic_index_in_dim(
                sums[k], 1 - mine(bit), left[k].index(bit), keepdims=False
            )
            sent[k] = swap(send, bit)
        for k in streams:
            bit = orders[k][step]
            keep = lax.dynamic_index_in_dim(sums[k], mine(bit), left[k].index(bit), keepdims=False)
            sums[k] = keep + sent[k]
            left[k].remove(bit)

    upper = mine(n_bits - 1) == 1
    last = [swap(jnp.where(upper, sums[c, 0], sums[c, 1]), n_bits - 1) for c in range(chunks)]
    done = [jnp.where(upper, sums[c, 1], sums[c, 0]) + last[c] for c in range(chunks)]
    total = jnp.concatenate(done, 0)
    row_coul = lax.dynamic_slice_in_dim(coulomb, ga_pos * half + band_pos * rows_dev, rows_dev, 0)
    weight = factor * jnp.sqrt(row_coul[:, None] * coulomb[None, :COLS])
    return jnp.stack([weight * total[:, :COLS], weight * total[:, COLS:]], 1)


def split(value):
    high = value.astype(jnp.bfloat16)
    return high, (value - high.astype(jnp.float32)).astype(jnp.bfloat16)


def kernel(
    rows_dev, m_ref, key_ref, fermi_ref, weight_ref, out_ref,
    slab, coef, ccol, right, cdef, own, got, left, rdef, part, got2, got3, got4,
    base_sem, slab_sem, fwd_sem, coef_sem, own_sem, m_sem, s2_sem, s3_sem, s4_sem,
):
    bands = m_ref.shape[1]
    width = rows_dev // CHUNKS
    tiles = width // LANES
    me = lax.axis_index("band")
    ga = lax.axis_index("ga")
    mine = [lax.rem(me // (1 << b), 2) for b in range(TOP + 1)]

    def across(b):
        return {"band": me + (1 - 2 * mine[b]) * (1 << b)}

    sibling = {"ga": 1 - ga}

    def rows_of(c, flips):
        dest = sum(((1 - mine[b]) if flips[b] else mine[b]) * (1 << b) for b in range(TOP + 1))
        return pl.ds(pl.multiple_of(dest * rows_dev + c * width, LANES), width)

    def flips_of(c, q, i, sent):
        first, second, third = ORDERS[c, q]
        return {BIT[first]: sent, BIT[second]: i // 2, BIT[third]: i % 2, TOP: q}

    def index(c, q, i):
        return (2 * c + q) * 4 + i

    def remote(src, dst, sems, k, device):
        return pltpu.make_async_remote_copy(
            src_ref=src, dst_ref=dst, send_sem=sems.at[0, k], recv_sem=sems.at[1, k],
            device_id=device, device_id_type=pl.DeviceIdType.MESH,
        )

    def base_copy():
        return remote(m_ref.at[:, :, pl.ds(0, COLS)], slab.at[0], base_sem, 0, sibling)

    def base_local():
        return pltpu.make_async_copy(m_ref.at[:, :, pl.ds(0, COLS)], slab.at[0], base_sem.at[0, 1])

    def slab_copy(b):
        k = SLOT[b]
        return remote(slab.at[0, ga], slab.at[k, ga], slab_sem, k - 1, across(BIT[b]))

    def slab_forward(b):
        k = SLOT[b]
        return remote(slab.at[k, ga], slab.at[k, ga], fwd_sem, k - 1, sibling)

    def coef_copy(b):
        k = SLOT[b]
        return remote(coef.at[0], coef.at[k], coef_sem, k - 1, across(BIT[b]))

    def m_copy(c, q, i):
        k = index(c, q, i)
        src = m_ref.at[:, :, rows_of(c, flips_of(c, q, i, 1))]
        return remote(src, got.at[k], m_sem, k, across(BIT[ORDERS[c, q][0]]))

    def own_copy(c, q, i):
        k = index(c, q, i)
        return pltpu.make_async_copy(
            m_ref.at[:, :, rows_of(c, flips_of(c, q, i, 0))], own.at[k], own_sem.at[k]
        )

    def s2_copy(c, q, r):
        k = (2 * c + q) * 2 + r
        return remote(part.at[index(c, q, 2 + r)], got2.at[k], s2_sem, k, across(BIT[ORDERS[c, q][1]]))

    def s3_copy(c, q):
        k = 2 * c + q
        return remote(part.at[index(c, q, 1)], got3.at[k], s3_sem, k, across(BIT[ORDERS[c, q][2]]))

    def s4_copy(c):
        return remote(part.at[index(c, 1, 0)], got4.at[c], s4_sem, c, across(TOP))

    firsts = sorted({o[0] for o in ORDERS.values()})

    @pl.when(ga == 0)
    def _():
        base_local().start()

    occ = (key_ref[...] < fermi_ref[0]).astype(jnp.float32)
    coef[0] = jnp.broadcast_to((0.5 - occ) * weight_ref[...], coef.shape[1:])

    barrier = pltpu.get_barrier_semaphore()
    for device in [across(b) for b in range(TOP + 1)] + [sibling]:
        pl.semaphore_signal(barrier, inc=1, device_id=device, device_id_type=pl.DeviceIdType.MESH)
    pl.semaphore_wait(barrier, TOP + 2)

    @pl.when(ga == 0)
    def _():
        base_copy().start()

    loads = [e[1:] for e in STEPS if e[0] == "m"]
    for e in loads:
        own_copy(*e).start()

    def prepare(k):
        column = jnp.broadcast_to(coef[k][0:1, :], (LANES, bands)).T
        ccol[k] = column
        for j in range(COLS // LANES):
            re_at, im_at = pl.ds(j * LANES, LANES), pl.ds(COLS + j * LANES, LANES)
            a, b = slab[k, 0, :, re_at], slab[k, 1, :, re_at]
            total = jnp.sum(column * (2.0 - a * a - b * b), 0, keepdims=True)
            cdef[k, :, re_at] = jnp.broadcast_to(0.5 * total, (8, LANES))
            cdef[k, :, im_at] = jnp.zeros((8, LANES), jnp.float32)
            for level, (sa, sb) in enumerate(zip(split(column * a), split(column * b))):
                right[k, level, :bands, re_at] = sa
                right[k, level, bands:, re_at] = sb
                right[k, level, :bands, im_at] = sb
                right[k, level, bands:, im_at] = -sa

    def dots(c, q, j):
        k = SLOT[ORDERS[c, q][0]]
        for i in range(2):
            blk = index(c, q, 2 * j + i)
            own_copy(c, q, 2 * j + i).wait()
            m_copy(c, q, 2 * j + i).wait_recv()
            for t in range(tiles):
                lanes = pl.ds(t * LANES, LANES)
                rows = pl.ds(i * width + t * LANES, LANES)
                total = jnp.zeros((1, LANES), jnp.float32)
                for ref, slot, at in ((own, 0, 0), (got, k, 2 * bands)):
                    a, b = ref[blk, 0, :, lanes], ref[blk, 1, :, lanes]
                    total += jnp.sum(ccol[slot] * (2.0 - a * a - b * b), 0, keepdims=True)
                    for level, (sa, sb) in enumerate(zip(split(a.T), split(b.T))):
                        left[level, rows, at : at + bands] = sa
                        left[level, rows, at + bands : at + 2 * bands] = sb
                rdef[rows, :] = jnp.broadcast_to(0.5 * total, (LANES, LANES)).T

        step = 2 * LANES

        def product(n, _):
            at = pl.ds(pl.multiple_of(n * step, step), step)
            acc = None
            for level, other in ((0, 0), (1, 0), (0, 1)):
                for slot, k_at in ((0, 0), (k, 2 * bands)):
                    term = jnp.dot(
                        left[level, :, k_at : k_at + 2 * bands],
                        right[slot, other, :, at],
                        preferred_element_type=jnp.float32,
                    )
                    acc = term if acc is None else acc + term
            keep = jnp.where(n * step < COLS, 1.0, 0.0)
            extra = rdef[...] * keep
            acc = acc + jnp.concatenate([extra, extra], 1)
            acc = acc + (cdef[0, 0:1, at] + cdef[k, 0:1, at])
            for i in range(2):
                part[index(c, q, 2 * j + i), :, at] = acc[i * width : (i + 1) * width]
            return 0

        lax.fori_loop(0, 2 * COLS // step, product, 0)

    flying = {"x": [], "y": [], "z": []}
    all_sends = []

    def send(link, copies):
        queue = flying[link]
        if len(queue) >= DEPTH:
            for copy in queue.pop(0):
                copy.wait_send()
        for copy in copies:
            copy.start()
        queue.append(copies)

    for e in STEPS:
        kind, rest = e[0], e[1:]
        if kind == "prep" and rest[0] == "o":
            @pl.when(ga == 0)
            def _():
                base_local().wait()
                base_copy().wait_send()

            @pl.when(ga == 1)
            def _():
                base_copy().wait_recv()

            prepare(0)
        elif kind == "slab":
            send(rest[0], [slab_copy(rest[0]), coef_copy(rest[0])])
        elif kind == "fwd":
            slab_copy(rest[0]).wait_recv()
            slab_forward(rest[0]).start()
        elif kind == "prep":
            slab_forward(rest[0]).wait()
            coef_copy(rest[0]).wait_recv()
            prepare(SLOT[rest[0]])
        elif kind == "m":
            send(ORDERS[rest[:2]][0], [m_copy(*rest)])
        elif kind == "dot":
            dots(*rest)
        elif kind == "s2":
            send(ORDERS[rest[:2]][1], [s2_copy(*rest)])
        elif kind == "a2":
            c, q, r = rest
            s2_copy(*rest).wait_recv()
            part[index(c, q, r)] += got2[(2 * c + q) * 2 + r]
        elif kind == "s3":
            send(ORDERS[rest[:2]][2], [s3_copy(*rest)])
        elif kind == "a3":
            c, q = rest
            s3_copy(*rest).wait_recv()
            part[index(c, q, 0)] += got3[2 * c + q]
        elif kind == "s4":
            send("z", [s4_copy(*rest)])
        elif kind == "a4":
            (c,) = rest
            s4_copy(c).wait_recv()
            out_ref[c * width : (c + 1) * width, :] = part[index(c, 0, 0)] + got4[c]

    for queue in flying.values():
        for copies in queue:
            for copy in copies:
                copy.wait_send()


def body_fast(matrix_elements, band_index, occupied, band_weight, coulomb):
    bands = matrix_elements.shape[1]
    half = matrix_elements.shape[2]
    n_band = lax.axis_size("band")
    rows_dev = half // n_band
    width = rows_dev // CHUNKS
    factor = 1.0 / math.sqrt(bands * n_band)
    f32 = jnp.float32
    any_spec = pl.BlockSpec(memory_space=pl.ANY)
    vmem_spec = pl.BlockSpec(memory_space=pltpu.VMEM)
    streams = 2 * CHUNKS
    dma = pltpu.SemaphoreType.DMA
    total = pl.pallas_call(
        functools.partial(kernel, rows_dev),
        out_shape=jax.ShapeDtypeStruct((rows_dev, 2 * COLS), f32),
        in_specs=[any_spec, vmem_spec, pl.BlockSpec(memory_space=pltpu.SMEM), vmem_spec],
        out_specs=vmem_spec,
        scratch_shapes=[
            pltpu.VMEM((4, 2, bands, COLS), f32),
            pltpu.VMEM((4, 8, bands), f32),
            pltpu.VMEM((4, bands, LANES), f32),
            pltpu.VMEM((4, 2, 2 * bands, 2 * COLS), jnp.bfloat16),
            pltpu.VMEM((4, 8, 2 * COLS), f32),
            pltpu.VMEM((4 * streams, 2, bands, width), f32),
            pltpu.VMEM((4 * streams, 2, bands, width), f32),
            pltpu.VMEM((2, 2 * width, 4 * bands), jnp.bfloat16),
            pltpu.VMEM((2 * width, LANES), f32),
            pltpu.VMEM((4 * streams, width, 2 * COLS), f32),
            pltpu.VMEM((2 * streams, width, 2 * COLS), f32),
            pltpu.VMEM((streams, width, 2 * COLS), f32),
            pltpu.VMEM((CHUNKS, width, 2 * COLS), f32),
            dma((2, 2)), dma((2, 3)), dma((2, 3)), dma((2, 3)), dma((4 * streams,)),
            dma((2, 4 * streams)), dma((2, 2 * streams)), dma((2, streams)), dma((2, CHUNKS)),
        ],
        compiler_params=pltpu.CompilerParams(
            collective_id=0, has_side_effects=True, vmem_limit_bytes=VMEM_BYTES
        ),
        name="reduce_sums",
    )(matrix_elements, band_index.reshape(1, bands), occupied, band_weight.reshape(1, bands))
    start = lax.axis_index("ga") * half + lax.axis_index("band") * rows_dev
    row_coul = lax.dynamic_slice_in_dim(coulomb, start, rows_dev, 0)
    weight = factor * jnp.sqrt(row_coul[:, None] * coulomb[None, :COLS])
    return jnp.stack([weight * total[:, :COLS], weight * total[:, COLS:]], 1)


def solution(mesh):
    n_band, n_ga = mesh.shape["band"], mesh.shape["ga"]

    def body(matrix_elements, *rest):
        rows_dev = matrix_elements.shape[2] // n_band
        aligned = rows_dev % (CHUNKS * LANES) == 0 and matrix_elements.shape[1] % LANES == 0
        if n_band == 2 << TOP and n_ga == 2 and aligned:
            return body_fast(matrix_elements, *rest)
        return body_plain(matrix_elements, *rest)

    return jax.shard_map(
        body,
        mesh=mesh,
        in_specs=(P(None, "band", "ga"), P("band"), P(), P("band"), P()),
        out_specs=P(("ga", "band"), None, None),
        check_vma=False,
    )
```

```python
import functools
import math

import jax
import jax.numpy as jnp
from jax import lax
from jax.experimental import pallas as pl
from jax.experimental.pallas import tpu as pltpu
from jax.sharding import PartitionSpec as P

COLS = 512
LANES = 128
CHUNKS = 3
DEPTH = 2
VMEM_BYTES = 67043328

X_BIT, Y_BIT, Z_BIT, S_BIT = 0, 1, 2, 3
BIT = {"x": X_BIT, "y": Y_BIT, "z": Z_BIT}
SLOT = {"x": 1, "y": 2, "z": 3}
LINE = ((0, 1), (1, 1), (1, 0), (0, 0))
LINE_SLOT = {(0, 1): 0, (1, 1): 1, (0, 0): 2}
LINE_SLOTS = 5
NEAR = {
    (0, 0, 1): "xy", (0, 1, 1): "yx", (0, 1, 0): "xy", (0, 0, 0): "yx", (1, 0, 1): "yx", (1, 1, 1): "xy",
    (1, 1, 0): "yx", (1, 0, 0): "xy",
}
FAR = {0: "xy", 1: "yx"}
STEPS = (
    ("m", 2, 1, 1), ("m", 0, 0, 1, 0), ("m", 2, 1, 3), ("m", 0, 1, 1, 0), ("m", 1, 0, 1, 0), ("m", 1, 1, 1, 0),
    ("prep", "o"), ("slab", "z"), ("slab", "x"), ("slab", "y"), ("m", 2, 1, 2), ("m", 0, 1, 0, 1), ("m", 0, 1, 1, 1),
    ("m", 2, 0, 3), ("m", 0, 0, 1, 1), ("m", 1, 0, 1, 1), ("fwd", "z"), ("fwd", "x"), ("fwd", "y"), ("prep", "z"),
    ("prep", "x"), ("prep", "y"), ("m", 2, 1, 0), ("m", 1, 0, 0, 1), ("m", 1, 1, 0, 1), ("dot", 2, 1, 1),
    ("dot", 0, 1, 1), ("s2", 0, 1, 1), ("s2", 2, 1, 1), ("m", 2, 0, 2), ("dot", 0, 0, 1), ("dot", 1, 0, 1),
    ("s2", 0, 0, 1), ("s2", 1, 0, 1), ("dot", 2, 1, 0), ("m", 2, 0, 0), ("m", 2, 0, 1), ("dot", 2, 0, 1),
    ("m", 1, 1, 1, 1), ("s2", 2, 1, 0), ("a2", 0, 1, 1), ("osend", 0, 1, 1), ("a2", 2, 1, 1), ("dot", 2, 0, 0),
    ("s3", 2, 1), ("m", 1, 1, 0, 0), ("a2", 1, 0, 1), ("osend", 1, 0, 1), ("a2", 0, 0, 1), ("osend", 0, 0, 1),
    ("m", 0, 1, 0, 0), ("iadd", 0, 0, 1), ("imid", 0, 0, 1), ("dot", 1, 1, 1), ("s2", 1, 1, 1), ("a2", 2, 1, 0),
    ("s2", 2, 0, 1), ("m", 0, 0, 0, 0), ("a3", 2, 1), ("osend2",), ("imid2", 1), ("dot", 1, 1, 0), ("s2", 1, 1, 0),
    ("dot", 0, 1, 0), ("s2", 0, 1, 0), ("iadd", 0, 1, 1), ("imid", 0, 1, 1), ("a2", 1, 1, 1), ("iadd", 1, 1, 1),
    ("imid", 1, 1, 1), ("osend", 1, 1, 1), ("iout2",), ("m", 1, 0, 0, 0), ("m", 0, 0, 0, 1), ("a2", 2, 0, 1),
    ("s2", 2, 0, 0), ("s3", 2, 0), ("a2", 1, 1, 0), ("osend", 1, 1, 0), ("a2", 0, 1, 0), ("imadd", 0, 1, 0),
    ("iout", 0), ("osend", 0, 1, 0), ("iadd", 1, 0, 1), ("imid", 1, 0, 1), ("dot", 1, 0, 0), ("s2", 1, 0, 0),
    ("imadd", 1, 1, 0), ("iout", 1), ("dot", 0, 0, 0), ("s2", 0, 0, 0), ("a2", 2, 0, 0), ("a3", 2, 0), ("imid2", 0),
    ("ofin2",), ("a2", 0, 0, 0), ("ofin", 0), ("a2", 1, 0, 0), ("iadd", 1, 0, 0), ("ifin", 1), ("ofin", 1),
    ("iadd", 0, 0, 0), ("ifin", 0), ("ifin2",),
)


def contract(left, right):
    return lax.dot_general(
        left,
        right,
        (((0,), (0,)), ((), ())),
        precision=lax.Precision.HIGH,
        preferred_element_type=jnp.float32,
    )


def right_side(slab):
    return jnp.concatenate(
        [jnp.concatenate([slab[0], slab[1]], 1), jnp.concatenate([slab[1], -slab[0]], 1)], 0
    )


def defects(coef, block):
    return jnp.sum(coef[:, None] * (2.0 - block[0] * block[0] - block[1] * block[1]), 0)


def body_plain(matrix_elements, band_index, occupied, band_weight, coulomb):
    bands_dev = matrix_elements.shape[1]
    half = matrix_elements.shape[2]
    n_band = lax.axis_size("band")
    n_bits = n_band.bit_length() - 1
    rows_dev = half // n_band
    n_ga = lax.axis_size("ga")
    chunks = 3 if rows_dev % 3 == 0 else 1
    width = rows_dev // chunks
    factor = 1.0 / math.sqrt(bands_dev * n_band)
    band_pos = lax.axis_index("band")
    ga_pos = lax.axis_index("ga")
    bits = list(range(n_bits - 1))
    top = n_band // 2
    firsts = [b % len(bits) for b in range(chunks)]
    streams = [(c, p) for p in range(2) for c in range(chunks)]
    orders = {}
    for c, p in streams:
        rest = bits[firsts[c] + 1 :] + bits[: firsts[c]]
        orders[c, p] = rest[p:] + rest[:p]

    def swap(x, bit):
        return lax.ppermute(x, "band", [(i, i ^ (1 << bit)) for i in range(n_band)])

    def mine(bit):
        return (band_pos >> bit) & 1

    def pick(x, c, p, which):
        bit = firsts[c]
        parts = []
        for d in range(p * top, (p + 1) * top):
            if not (d >> bit) & 1:
                low = d * rows_dev + c * width
                high = (d | (1 << bit)) * rows_dev + c * width
                parts.append(
                    jnp.where(which == 1, x[..., high : high + width], x[..., low : low + width])
                )
        return jnp.concatenate(parts, -1)

    there = {
        (c, p): swap(pick(matrix_elements, c, p, 1 - mine(firsts[c])), firsts[c])
        for c, p in streams
    }

    occ = (band_index < occupied[0]).astype(jnp.float32)
    coef = (0.5 - occ) * band_weight
    first = matrix_elements[:, :, :COLS]
    moved = lax.ppermute(first, "ga", [(0, g) for g in range(1, n_ga)][:1])
    slab = jnp.where(ga_pos == 0, first, moved)
    scaled = coef[None, :, None] * slab
    right = right_side(scaled)
    rights = [right_side(swap(scaled, bit)) for bit in firsts]
    row_def = defects(coef, matrix_elements)
    col_def = defects(coef, slab)

    sums, left = {}, {}
    for c, p in streams:
        bit = firsts[c]
        rows_here = pick(row_def, c, p, mine(bit))
        send = jnp.concatenate([pick(row_def, c, p, 1 - mine(bit)), col_def])
        got = swap(send, bit)
        count = rows_here.shape[0]
        rows_sum = rows_here + got[:count]
        cols_sum = col_def + got[count:]
        here = pick(matrix_elements, c, p, mine(bit))
        part = contract(here.reshape(2 * bands_dev, count), right)
        part = part + contract(there[c, p].reshape(2 * bands_dev, count), rights[c])
        extra = 0.5 * (rows_sum[:, None] + cols_sum[None, :])
        part = part + jnp.concatenate([extra, jnp.zeros_like(extra)], 1)
        sums[c, p] = part.reshape((2,) * (n_bits - 2) + (width, 2 * COLS))
        left[c, p] = [b for b in reversed(bits) if b != bit]

    for step in range(n_bits - 2):
        sent = {}
        for k in streams:
            bit = orders[k][step]
            send = lax.dynamic_index_in_dim(
                sums[k], 1 - mine(bit), left[k].index(bit), keepdims=False
            )
            sent[k] = swap(send, bit)
        for k in streams:
            bit = orders[k][step]
            keep = lax.dynamic_index_in_dim(sums[k], mine(bit), left[k].index(bit), keepdims=False)
            sums[k] = keep + sent[k]
            left[k].remove(bit)

    upper = mine(n_bits - 1) == 1
    last = [swap(jnp.where(upper, sums[c, 0], sums[c, 1]), n_bits - 1) for c in range(chunks)]
    done = [jnp.where(upper, sums[c, 1], sums[c, 0]) + last[c] for c in range(chunks)]
    total = jnp.concatenate(done, 0)
    row_coul = lax.dynamic_slice_in_dim(coulomb, ga_pos * half + band_pos * rows_dev, rows_dev, 0)
    weight = factor * jnp.sqrt(row_coul[:, None] * coulomb[None, :COLS])
    return jnp.stack([weight * total[:, :COLS], weight * total[:, COLS:]], 1)


def split(value):
    high = value.astype(jnp.bfloat16)
    return high, (value - high.astype(jnp.float32)).astype(jnp.bfloat16)


def kernel(
    rows_dev, factor, m_ref, key_ref, fermi_ref, weight_ref, coul_ref, out_ref,
    keys, weights, coul, rowc, slab, coef, ccol, right, cdef, own, got, left, rdef, part, got2, got3, line,
    small_sem, base_sem, slab_sem, fwd_sem, coef_sem, own_sem, m_sem, s2_sem, s3_sem, line_sem,
):
    bands, half = m_ref.shape[1], m_ref.shape[2]
    width = rows_dev // CHUNKS
    tiles = width // LANES
    me = lax.axis_index("band")
    ga = lax.axis_index("ga")
    mine = [lax.rem(me // (1 << b), 2) for b in range(4)]

    def flip(bit, by):
        return bit + by - 2 * bit * by

    inner = flip(mine[Z_BIT], mine[S_BIT])

    def across(*bits):
        return {"band": me + sum((1 - 2 * mine[b]) * (1 << b) for b in bits)}

    device = {"x": across(X_BIT), "y": across(Y_BIT), "z": across(Z_BIT), "m": across(Z_BIT, S_BIT)}
    sibling = {"ga": 1 - ga}

    def rows_of(c, flips):
        dest = sum(flip(mine[b], flips[b]) * (1 << b) for b in range(4))
        return pl.ds(pl.multiple_of(dest * rows_dev + c * width, LANES), width)

    far_base = 8 * len(LINE) // 2

    def near(c, o, s):
        return c * len(LINE) + LINE.index((o, s))

    def block(*name):
        if len(name) == 4:
            return 2 * near(*name[:3]) + name[3]
        return far_base + 4 * name[1] + name[2]

    def m_rows(sent, *name):
        if len(name) == 4:
            c, o, s, i = name
            first, second = NEAR[c, o, s]
            return rows_of(c, {BIT[first]: sent, BIT[second]: i, Z_BIT: o ^ s, S_BIT: s})
        c, k, i = name
        second, third = FAR[k]
        o, s = (1 - k, 1 - inner) if sent else (k, inner)
        return rows_of(c, {BIT[second]: i // 2, BIT[third]: i % 2, Z_BIT: flip(s, o), S_BIT: s})

    def first_link(name):
        return NEAR[name[:3]][0] if len(name) == 4 else "z"

    def remote(src, dst, sems, k, to):
        return pltpu.make_async_remote_copy(
            src_ref=src, dst_ref=dst, send_sem=sems.at[0, k], recv_sem=sems.at[1, k],
            device_id=to, device_id_type=pl.DeviceIdType.MESH,
        )

    def base_copy():
        return remote(m_ref.at[:, :, pl.ds(0, COLS)], slab.at[0], base_sem, 0, sibling)

    def base_local():
        return pltpu.make_async_copy(m_ref.at[:, :, pl.ds(0, COLS)], slab.at[0], base_sem.at[0, 1])

    def slab_copy(b):
        k = SLOT[b]
        return remote(slab.at[0, ga], slab.at[k, ga], slab_sem, k - 1, device[b])

    def slab_forward(b):
        k = SLOT[b]
        return remote(slab.at[k, ga], slab.at[k, ga], fwd_sem, k - 1, sibling)

    def coef_copy(b):
        k = SLOT[b]
        return remote(coef.at[0], coef.at[k], coef_sem, k - 1, device[b])

    def m_copy(*name):
        k = block(*name)
        return remote(m_ref.at[:, :, m_rows(1, *name)], got.at[k], m_sem, k, device[first_link(name)])

    def own_copy(*name):
        k = block(*name)
        return pltpu.make_async_copy(m_ref.at[:, :, m_rows(0, *name)], own.at[k], own_sem.at[k])

    def s2_of(name):
        if name[0] < 2:
            k = near(*name)
            return NEAR[name][1], k, block(*name, 1), block(*name, 0)
        c, k, r = name
        return FAR[k][0], far_base // 2 + 2 * k + r, block(c, k, 2 + r), block(c, k, r)

    def s2_copy(name):
        link, k, sent, _ = s2_of(name)
        return remote(part.at[sent], got2.at[k], s2_sem, k, device[link])

    def s3_copy(c, k):
        return remote(part.at[block(c, k, 1)], got3.at[k], s3_sem, k, device[FAR[k][1]])

    far_line = 2 * LINE_SLOTS

    def line_copy(src, slot, link):
        return remote(src, line.at[slot], line_sem, slot, device[link])

    def end_slot(c, o, s):
        return c * LINE_SLOTS + LINE_SLOT[o, s]

    def mid_slot(c, o):
        return c * LINE_SLOTS + 3 + o

    small = [
        pltpu.make_async_copy(src, dst, small_sem.at[i])
        for i, (src, dst) in enumerate(((key_ref, keys), (weight_ref, weights), (coul_ref, coul)))
    ]
    barrier = pltpu.get_barrier_semaphore()

    def greet(to):
        pl.semaphore_signal(barrier, inc=1, device_id=to, device_id_type=pl.DeviceIdType.MESH)

    for to in (device["x"], device["y"], device["z"], sibling):
        greet(to)

    @pl.when(inner == 1)
    def _():
        greet(device["m"])

    for copy in small:
        copy.start()

    @pl.when(ga == 0)
    def _():
        base_local().start()

    pl.semaphore_wait(barrier, 4 + inner)

    @pl.when(ga == 0)
    def _():
        base_copy().start()

    def prepare(k):
        column = jnp.broadcast_to(coef[k][0:1, :], (LANES, bands)).T
        ccol[k] = column
        for j in range(COLS // LANES):
            re_at, im_at = pl.ds(j * LANES, LANES), pl.ds(COLS + j * LANES, LANES)
            a, b = slab[k, 0, :, re_at], slab[k, 1, :, re_at]
            total = jnp.sum(column * (2.0 - a * a - b * b), 0, keepdims=True)
            cdef[k, :, re_at] = jnp.broadcast_to(0.5 * total, (8, LANES))
            cdef[k, :, im_at] = jnp.zeros((8, LANES), jnp.float32)
            for level, (sa, sb) in enumerate(zip(split(column * a), split(column * b))):
                right[k, level, :bands, re_at] = sa
                right[k, level, bands:, re_at] = sb
                right[k, level, :bands, im_at] = sb
                right[k, level, bands:, im_at] = -sa

    def prepare_own():
        for copy in small:
            copy.wait()
        occ = (keys[...] < fermi_ref[0]).astype(jnp.float32)
        coef[0] = jnp.broadcast_to((0.5 - occ) * weights[...], coef.shape[1:])
        for t in range(CHUNKS * tiles):
            at = pl.multiple_of(ga * half + me * rows_dev + t * LANES, LANES)
            rowc[t] = jnp.broadcast_to(coul[0:1, pl.ds(at, LANES)], (LANES, LANES)).T

        @pl.when(ga == 0)
        def _():
            base_local().wait()
            base_copy().wait_send()

        @pl.when(ga == 1)
        def _():
            base_copy().wait_recv()

        prepare(0)

    def dots(slot, names):
        for i, name in enumerate(names):
            blk = block(*name)
            own_copy(*name).wait()
            m_copy(*name).wait_recv()
            for t in range(tiles):
                lanes = pl.ds(t * LANES, LANES)
                rows = pl.ds(i * width + t * LANES, LANES)
                total = jnp.zeros((1, LANES), jnp.float32)
                for ref, k, at in ((own, 0, 0), (got, slot, 2 * bands)):
                    a, b = ref[blk, 0, :, lanes], ref[blk, 1, :, lanes]
                    total += jnp.sum(ccol[k] * (2.0 - a * a - b * b), 0, keepdims=True)
                    for level, (sa, sb) in enumerate(zip(split(a.T), split(b.T))):
                        left[level, rows, at : at + bands] = sa
                        left[level, rows, at + bands : at + 2 * bands] = sb
                rdef[rows, :] = jnp.broadcast_to(0.5 * total, (LANES, LANES)).T

        step = 2 * LANES

        def product(n, _):
            at = pl.ds(pl.multiple_of(n * step, step), step)
            acc = None
            for level, other in ((0, 0), (1, 0), (0, 1)):
                for k, k_at in ((0, 0), (slot, 2 * bands)):
                    term = jnp.dot(
                        left[level, :, k_at : k_at + 2 * bands],
                        right[k, other, :, at],
                        preferred_element_type=jnp.float32,
                    )
                    acc = term if acc is None else acc + term
            keep = jnp.where(n * step < COLS, 1.0, 0.0)
            extra = rdef[...] * keep
            acc = acc + jnp.concatenate([extra, extra], 1)
            acc = acc + (cdef[0, 0:1, at] + cdef[slot, 0:1, at])
            for i, name in enumerate(names):
                part[block(*name), :, at] = acc[i * width : (i + 1) * width]
            return 0

        lax.fori_loop(0, 2 * COLS // step, product, 0)

    def finish(c, one, two):
        for t in range(tiles):
            rows = pl.ds(t * LANES, LANES)
            at = pl.ds(c * width + t * LANES, LANES)
            wide = jnp.concatenate([rowc[c * tiles + t]] * (COLS // LANES), 1)
            weight = factor * jnp.sqrt(wide * coul[0:1, :COLS])
            for p in range(2):
                cols = pl.ds(p * COLS, COLS)
                out_ref[at, p, :] = weight * (one[rows, cols] + two[rows, cols])

    flying = {}

    def only(cls, action):
        if cls == "B":
            action()
        else:
            pl.when(inner == (1 if cls == "I" else 0))(action)

    def wait_sent(copies):
        for make in copies:
            make().wait_send()

    def send(cls, link, *copies):
        entry = list(copies)
        waits = {}
        for c in "OI" if cls == "B" else cls:
            queue = flying.setdefault((c, link), [])
            if len(queue) >= DEPTH:
                waits[c] = queue.pop(0)
            queue.append(entry)
        if len(waits) == 2 and waits["O"] is waits["I"]:
            wait_sent(waits["O"])
            waits = {}
        for c, copies in waits.items():
            only(c, functools.partial(wait_sent, copies))

        def start():
            for make in entry:
                make().start()

        only(cls, start)

    def add(cls, copy, blk, ref, k):
        def action():
            copy().wait_recv()
            part[blk] += ref[k]

        only(cls, action)

    def do(f, *args):
        return functools.partial(f, *args)

    loads = [e[1:] for e in STEPS if e[0] == "m"]
    for e in STEPS:
        kind, rest = e[0], e[1:]
        if kind == "prep" and rest[0] == "o":
            for name in loads:
                own_copy(*name).start()
            prepare_own()
        elif kind == "slab":
            send("B", rest[0], do(slab_copy, *rest), do(coef_copy, *rest))
        elif kind == "fwd":
            slab_copy(*rest).wait_recv()
            slab_forward(*rest).start()
        elif kind == "prep":
            slab_forward(*rest).wait()
            coef_copy(*rest).wait_recv()
            prepare(SLOT[rest[0]])
        elif kind == "m":
            send("B", first_link(rest), do(m_copy, *rest))
        elif kind == "dot" and len(rest) == 3 and rest[0] < 2:
            dots(SLOT[NEAR[rest][0]], [rest + (i,) for i in range(2)])
        elif kind == "dot":
            c, k, j = rest
            dots(SLOT["z"], [(c, k, 2 * j + i) for i in range(2)])
        elif kind == "s2":
            send("B", s2_of(rest)[0], do(s2_copy, rest))
        elif kind == "a2":
            _, k, _, blk = s2_of(rest)
            add("B", do(s2_copy, rest), blk, got2, k)
        elif kind == "s3":
            send("B", FAR[rest[1]][1], do(s3_copy, *rest))
        elif kind == "a3":
            add("B", do(s3_copy, *rest), block(*rest, 0), got3, rest[1])
        elif kind == "osend":
            c, o, s = rest
            slot = end_slot(c, 1 - o, s)
            send("O", "z", do(line_copy, part.at[block(*rest, 0)], slot, "z"))
        elif kind == "iadd":
            slot = end_slot(*rest)
            add("I", do(line_copy, line.at[slot], slot, "z"), block(*rest, 0), line, slot)
        elif kind == "imid":
            c, o, s = rest
            send("I", "m", do(line_copy, part.at[block(*rest, 0)], mid_slot(c, o), "m"))
        elif kind == "imadd":
            slot = mid_slot(rest[0], 1)
            add("I", do(line_copy, line.at[slot], slot, "m"), block(*rest, 0), line, slot)
        elif kind == "iout":
            (c,) = rest
            send("I", "z", do(line_copy, part.at[block(c, 1, 0, 0)], c * LINE_SLOTS, "z"))
        elif kind in ("ifin", "ofin"):
            (c,) = rest
            slot, link = (mid_slot(c, 0), "m") if kind == "ifin" else (c * LINE_SLOTS, "z")

            def action(c=c, slot=slot, link=link):
                line_copy(line.at[slot], slot, link).wait_recv()
                finish(c, part.at[block(c, 0, 0, 0)], line.at[slot])

            only("I" if kind == "ifin" else "O", action)
        elif kind == "imid2":
            (k,) = rest
            send("I", "m", do(line_copy, part.at[block(2, k, 0)], far_line + 1 + k, "m"))
        elif kind == "osend2":
            send("O", "z", do(line_copy, part.at[block(2, 1, 0)], far_line, "z"))
        elif kind == "iout2":
            def arrived():
                line_copy(line.at[far_line + 2], far_line + 2, "m").wait_recv()

            only("I", arrived)
            send("I", "z", do(line_copy, line.at[far_line + 2], far_line, "z"))
        elif kind == "ifin2":
            def action():
                line_copy(line.at[far_line + 1], far_line + 1, "m").wait_recv()
                line_copy(line.at[far_line], far_line, "z").wait_recv()
                finish(2, line.at[far_line], line.at[far_line + 1])

            only("I", action)
        elif kind == "ofin2":
            def action():
                line_copy(line.at[far_line], far_line, "z").wait_recv()
                finish(2, part.at[block(2, 0, 0)], line.at[far_line])

            only("O", action)

    for c in "OI":
        def drain(c=c):
            for (cls, _), queue in flying.items():
                for copies in queue if cls == c else ():
                    wait_sent(copies)

        only(c, drain)


def body_fast(matrix_elements, band_index, occupied, band_weight, coulomb):
    bands = matrix_elements.shape[1]
    half = matrix_elements.shape[2]
    n_band = lax.axis_size("band")
    rows_dev = half // n_band
    width = rows_dev // CHUNKS
    factor = 1.0 / math.sqrt(bands * n_band)
    f32 = jnp.float32
    hbm = pl.BlockSpec(memory_space=pl.ANY)
    blocks = 8 * CHUNKS
    near_streams = 2 * len(LINE)
    dma = pltpu.SemaphoreType.DMA
    return pl.pallas_call(
        functools.partial(kernel, rows_dev, factor),
        out_shape=jax.ShapeDtypeStruct((rows_dev, 2, COLS), f32),
        in_specs=[hbm, hbm, pl.BlockSpec(memory_space=pltpu.SMEM), hbm, hbm],
        out_specs=pl.BlockSpec(memory_space=pltpu.VMEM),
        scratch_shapes=[
            pltpu.VMEM((1, bands), jnp.int32),
            pltpu.VMEM((1, bands), f32),
            pltpu.VMEM((1, coulomb.shape[0]), f32),
            pltpu.VMEM((rows_dev // LANES, LANES, LANES), f32),
            pltpu.VMEM((4, 2, bands, COLS), f32),
            pltpu.VMEM((4, 8, bands), f32),
            pltpu.VMEM((4, bands, LANES), f32),
            pltpu.VMEM((4, 2, 2 * bands, 2 * COLS), jnp.bfloat16),
            pltpu.VMEM((4, 8, 2 * COLS), f32),
            pltpu.VMEM((blocks, 2, bands, width), f32),
            pltpu.VMEM((blocks, 2, bands, width), f32),
            pltpu.VMEM((2, 2 * width, 4 * bands), jnp.bfloat16),
            pltpu.VMEM((2 * width, LANES), f32),
            pltpu.VMEM((blocks, width, 2 * COLS), f32),
            pltpu.VMEM((near_streams + 4, width, 2 * COLS), f32),
            pltpu.VMEM((2, width, 2 * COLS), f32),
            pltpu.VMEM((2 * LINE_SLOTS + 3, width, 2 * COLS), f32),
            dma((3,)), dma((2, 2)), dma((2, 3)), dma((2, 3)), dma((2, 3)), dma((blocks,)),
            dma((2, blocks)), dma((2, near_streams + 4)), dma((2, 2)), dma((2, 2 * LINE_SLOTS + 3)),
        ],
        compiler_params=pltpu.CompilerParams(
            collective_id=0, has_side_effects=True, vmem_limit_bytes=VMEM_BYTES
        ),
        name="reduce_sums",
    )(
        matrix_elements, band_index.reshape(1, bands), occupied, band_weight.reshape(1, bands),
        coulomb.reshape(1, coulomb.shape[0]),
    )


def solution(mesh):
    n_band, n_ga = mesh.shape["band"], mesh.shape["ga"]

    def body(matrix_elements, *rest):
        rows_dev = matrix_elements.shape[2] // n_band
        aligned = rows_dev % (CHUNKS * LANES) == 0 and matrix_elements.shape[1] % LANES == 0
        if n_band == 1 << len(LINE) and n_ga == 2 and aligned:
            return body_fast(matrix_elements, *rest)
        return body_plain(matrix_elements, *rest)

    return jax.shard_map(
        body,
        mesh=mesh,
        in_specs=(P(None, "band", "ga"), P("band"), P(), P("band"), P()),
        out_specs=P(("ga", "band"), None, None),
        check_vma=False,
    )
```

```python
import functools
import math

import jax
import jax.numpy as jnp
from jax import lax
from jax.experimental import pallas as pl
from jax.experimental.pallas import tpu as pltpu
from jax.sharding import PartitionSpec as P

COLS = 512
LANES = 128
CHUNKS = 3
DEPTH = 2
VMEM_BYTES = 67043328

X_BIT, Y_BIT, Z_BIT, S_BIT = 0, 1, 2, 3
BIT = {"x": X_BIT, "y": Y_BIT, "z": Z_BIT}
SLOT = {"x": 1, "y": 2, "z": 3}
LINE = ((0, 1), (1, 1), (1, 0), (0, 0))
LINE_SLOT = {(0, 1): 0, (1, 1): 1, (0, 0): 2}
LINE_SLOTS = 5
PIECES = 4
NEAR = {
    (0, 0, 1): "xy", (0, 1, 1): "yx", (0, 1, 0): "xy", (0, 0, 0): "yx", (1, 0, 1): "yx", (1, 1, 1): "xy",
    (1, 1, 0): "yx", (1, 0, 0): "xy",
}
FAR = {0: "xy", 1: "yx"}
STEPS = (
    ("m", 2, 1, 1), ("m", 0, 0, 1, 0), ("m", 2, 1, 3), ("m", 0, 1, 1, 0), ("m", 1, 0, 1, 0), ("m", 1, 1, 1, 0),
    ("prep", "o"), ("slab", "z"), ("slab", "x"), ("slab", "y"), ("m", 2, 1, 2), ("m", 0, 1, 0, 1), ("m", 0, 1, 1, 1),
    ("m", 2, 0, 3), ("m", 0, 0, 1, 1), ("m", 1, 0, 1, 1), ("fwd", "z"), ("fwd", "x"), ("fwd", "y"), ("prep", "z"),
    ("prep", "x"), ("prep", "y"), ("m", 2, 1, 0), ("m", 1, 0, 0, 1), ("m", 1, 1, 0, 1), ("dot", 2, 1, 1),
    ("dot", 0, 1, 1), ("s2", 0, 1, 1), ("s2", 2, 1, 1), ("m", 2, 0, 2), ("dot", 0, 0, 1), ("dot", 1, 0, 1),
    ("s2", 0, 0, 1), ("s2", 1, 0, 1), ("dot", 2, 1, 0), ("m", 2, 0, 0), ("m", 2, 0, 1), ("dot", 2, 0, 1),
    ("m", 1, 1, 1, 1), ("s2", 2, 1, 0), ("a2", 0, 1, 1), ("osend", 0, 1, 1), ("a2", 2, 1, 1), ("dot", 2, 0, 0),
    ("s3", 2, 1), ("m", 1, 1, 0, 0), ("a2", 1, 0, 1), ("osend", 1, 0, 1), ("a2", 0, 0, 1), ("osend", 0, 0, 1),
    ("m", 0, 1, 0, 0), ("iadd", 0, 0, 1), ("imid", 0, 0, 1), ("dot", 1, 1, 1), ("s2", 1, 1, 1), ("a2", 2, 1, 0),
    ("s2", 2, 0, 1), ("m", 0, 0, 0, 0), ("a3", 2, 1), ("osend2",), ("imid2", 1), ("dot", 1, 1, 0), ("s2", 1, 1, 0),
    ("dot", 0, 1, 0), ("s2", 0, 1, 0), ("iadd", 0, 1, 1), ("imid", 0, 1, 1), ("a2", 1, 1, 1), ("iadd", 1, 1, 1),
    ("imid", 1, 1, 1), ("osend", 1, 1, 1), ("iout2",), ("m", 1, 0, 0, 0), ("m", 0, 0, 0, 1), ("a2", 2, 0, 1),
    ("s2", 2, 0, 0), ("s3", 2, 0), ("a2", 1, 1, 0), ("osend", 1, 1, 0), ("a2", 0, 1, 0), ("imadd", 0, 1, 0),
    ("iout", 0), ("osend", 0, 1, 0), ("iadd", 1, 0, 1), ("imid", 1, 0, 1), ("dot", 1, 0, 0), ("s2", 1, 0, 0),
    ("imadd", 1, 1, 0), ("iout", 1), ("dot", 0, 0, 0), ("s2", 0, 0, 0), ("a2", 2, 0, 0), ("a3", 2, 0), ("imid2", 0),
    ("ofin2",), ("a2", 0, 0, 0), ("ofin", 0), ("a2", 1, 0, 0), ("iadd", 1, 0, 0), ("ifin", 1), ("ofin", 1),
    ("iadd", 0, 0, 0), ("ifin", 0), ("ifin2",),
)


def contract(left, right):
    return lax.dot_general(
        left,
        right,
        (((0,), (0,)), ((), ())),
        precision=lax.Precision.HIGH,
        preferred_element_type=jnp.float32,
    )


def right_side(slab):
    return jnp.concatenate(
        [jnp.concatenate([slab[0], slab[1]], 1), jnp.concatenate([slab[1], -slab[0]], 1)], 0
    )


def defects(coef, block):
    return jnp.sum(coef[:, None] * (2.0 - block[0] * block[0] - block[1] * block[1]), 0)


def body_plain(matrix_elements, band_index, occupied, band_weight, coulomb):
    bands_dev = matrix_elements.shape[1]
    half = matrix_elements.shape[2]
    n_band = lax.axis_size("band")
    n_bits = n_band.bit_length() - 1
    rows_dev = half // n_band
    n_ga = lax.axis_size("ga")
    chunks = 3 if rows_dev % 3 == 0 else 1
    width = rows_dev // chunks
    factor = 1.0 / math.sqrt(bands_dev * n_band)
    band_pos = lax.axis_index("band")
    ga_pos = lax.axis_index("ga")
    bits = list(range(n_bits - 1))
    top = n_band // 2
    firsts = [b % len(bits) for b in range(chunks)]
    streams = [(c, p) for p in range(2) for c in range(chunks)]
    orders = {}
    for c, p in streams:
        rest = bits[firsts[c] + 1 :] + bits[: firsts[c]]
        orders[c, p] = rest[p:] + rest[:p]

    def swap(x, bit):
        return lax.ppermute(x, "band", [(i, i ^ (1 << bit)) for i in range(n_band)])

    def mine(bit):
        return (band_pos >> bit) & 1

    def pick(x, c, p, which):
        bit = firsts[c]
        parts = []
        for d in range(p * top, (p + 1) * top):
            if not (d >> bit) & 1:
                low = d * rows_dev + c * width
                high = (d | (1 << bit)) * rows_dev + c * width
                parts.append(
                    jnp.where(which == 1, x[..., high : high + width], x[..., low : low + width])
                )
        return jnp.concatenate(parts, -1)

    there = {
        (c, p): swap(pick(matrix_elements, c, p, 1 - mine(firsts[c])), firsts[c])
        for c, p in streams
    }

    occ = (band_index < occupied[0]).astype(jnp.float32)
    coef = (0.5 - occ) * band_weight
    first = matrix_elements[:, :, :COLS]
    moved = lax.ppermute(first, "ga", [(0, g) for g in range(1, n_ga)][:1])
    slab = jnp.where(ga_pos == 0, first, moved)
    scaled = coef[None, :, None] * slab
    right = right_side(scaled)
    rights = [right_side(swap(scaled, bit)) for bit in firsts]
    row_def = defects(coef, matrix_elements)
    col_def = defects(coef, slab)

    sums, left = {}, {}
    for c, p in streams:
        bit = firsts[c]
        rows_here = pick(row_def, c, p, mine(bit))
        send = jnp.concatenate([pick(row_def, c, p, 1 - mine(bit)), col_def])
        got = swap(send, bit)
        count = rows_here.shape[0]
        rows_sum = rows_here + got[:count]
        cols_sum = col_def + got[count:]
        here = pick(matrix_elements, c, p, mine(bit))
        part = contract(here.reshape(2 * bands_dev, count), right)
        part = part + contract(there[c, p].reshape(2 * bands_dev, count), rights[c])
        extra = 0.5 * (rows_sum[:, None] + cols_sum[None, :])
        part = part + jnp.concatenate([extra, jnp.zeros_like(extra)], 1)
        sums[c, p] = part.reshape((2,) * (n_bits - 2) + (width, 2 * COLS))
        left[c, p] = [b for b in reversed(bits) if b != bit]

    for step in range(n_bits - 2):
        sent = {}
        for k in streams:
            bit = orders[k][step]
            send = lax.dynamic_index_in_dim(
                sums[k], 1 - mine(bit), left[k].index(bit), keepdims=False
            )
            sent[k] = swap(send, bit)
        for k in streams:
            bit = orders[k][step]
            keep = lax.dynamic_index_in_dim(sums[k], mine(bit), left[k].index(bit), keepdims=False)
            sums[k] = keep + sent[k]
            left[k].remove(bit)

    upper = mine(n_bits - 1) == 1
    last = [swap(jnp.where(upper, sums[c, 0], sums[c, 1]), n_bits - 1) for c in range(chunks)]
    done = [jnp.where(upper, sums[c, 1], sums[c, 0]) + last[c] for c in range(chunks)]
    total = jnp.concatenate(done, 0)
    row_coul = lax.dynamic_slice_in_dim(coulomb, ga_pos * half + band_pos * rows_dev, rows_dev, 0)
    weight = factor * jnp.sqrt(row_coul[:, None] * coulomb[None, :COLS])
    return jnp.stack([weight * total[:, :COLS], weight * total[:, COLS:]], 1)


def split(value):
    high = value.astype(jnp.bfloat16)
    return high, (value - high.astype(jnp.float32)).astype(jnp.bfloat16)


def kernel(
    rows_dev, m_ref, key_ref, fermi_ref, weight_ref, coul_ref, out_ref,
    done, keys, weights, coul, rowc, slab, coef, ccol, right, cdef, own, got, left, rdef, part, got2, got3, line,
    small_sem, base_sem, slab_sem, fwd_sem, coef_sem, own_sem, m_sem, s2_sem, s3_sem, line_sem, out_sem,
):
    bands, half = m_ref.shape[1], m_ref.shape[2]
    width = rows_dev // CHUNKS
    tiles = width // LANES
    me = lax.axis_index("band")
    ga = lax.axis_index("ga")
    mine = [lax.rem(me // (1 << b), 2) for b in range(4)]

    def flip(bit, by):
        return bit + by - 2 * bit * by

    inner = flip(mine[Z_BIT], mine[S_BIT])

    def across(*bits):
        return {"band": me + sum((1 - 2 * mine[b]) * (1 << b) for b in bits)}

    device = {"x": across(X_BIT), "y": across(Y_BIT), "z": across(Z_BIT), "m": across(Z_BIT, S_BIT)}
    sibling = {"ga": 1 - ga}

    def rows_of(c, flips):
        dest = sum(flip(mine[b], flips[b]) * (1 << b) for b in range(4))
        return pl.ds(pl.multiple_of(dest * rows_dev + c * width, LANES), width)

    far_base = 8 * len(LINE) // 2

    def near(c, o, s):
        return c * len(LINE) + LINE.index((o, s))

    def block(*name):
        if len(name) == 4:
            return 2 * near(*name[:3]) + name[3]
        return far_base + 4 * name[1] + name[2]

    def m_rows(sent, *name):
        if len(name) == 4:
            c, o, s, i = name
            first, second = NEAR[c, o, s]
            return rows_of(c, {BIT[first]: sent, BIT[second]: i, Z_BIT: o ^ s, S_BIT: s})
        c, k, i = name
        second, third = FAR[k]
        o, s = (1 - k, 1 - inner) if sent else (k, inner)
        return rows_of(c, {BIT[second]: i // 2, BIT[third]: i % 2, Z_BIT: flip(s, o), S_BIT: s})

    def first_link(name):
        return NEAR[name[:3]][0] if len(name) == 4 else "z"

    def remote(src, dst, sems, k, to):
        return pltpu.make_async_remote_copy(
            src_ref=src, dst_ref=dst, send_sem=sems.at[0, k], recv_sem=sems.at[1, k],
            device_id=to, device_id_type=pl.DeviceIdType.MESH,
        )

    def base_copy():
        return remote(m_ref.at[:, :, pl.ds(0, COLS)], slab.at[0], base_sem, 0, sibling)

    def base_local():
        return pltpu.make_async_copy(m_ref.at[:, :, pl.ds(0, COLS)], slab.at[0], base_sem.at[0, 1])

    def slab_copy(b):
        k = SLOT[b]
        return remote(slab.at[0, ga], slab.at[k, ga], slab_sem, k - 1, device[b])

    def slab_forward(b):
        k = SLOT[b]
        return remote(slab.at[k, ga], slab.at[k, ga], fwd_sem, k - 1, sibling)

    def coef_copy(b):
        k = SLOT[b]
        return remote(coef.at[0], coef.at[k], coef_sem, k - 1, device[b])

    def m_copy(*name):
        k = block(*name)
        return remote(m_ref.at[:, :, m_rows(1, *name)], got.at[k], m_sem, k, device[first_link(name)])

    def own_copy(*name):
        k = block(*name)
        return pltpu.make_async_copy(m_ref.at[:, :, m_rows(0, *name)], own.at[k], own_sem.at[k])

    def s2_of(name):
        if name[0] < 2:
            k = near(*name)
            return NEAR[name][1], k, block(*name, 1), block(*name, 0)
        c, k, r = name
        return FAR[k][0], far_base // 2 + 2 * k + r, block(c, k, 2 + r), block(c, k, r)

    def s2_copy(name):
        link, k, sent, _ = s2_of(name)
        return remote(part.at[sent], got2.at[k], s2_sem, k, device[link])

    def s3_copy(c, k):
        return remote(part.at[block(c, k, 1)], got3.at[k], s3_sem, k, device[FAR[k][1]])

    far_line = 2 * LINE_SLOTS

    def line_copy(src, slot, link):
        return remote(src, line.at[slot], line_sem, slot, device[link])

    def end_slot(c, o, s):
        return c * LINE_SLOTS + LINE_SLOT[o, s]

    def mid_slot(c, o):
        return c * LINE_SLOTS + 3 + o

    small = [
        pltpu.make_async_copy(src, dst, small_sem.at[i])
        for i, (src, dst) in enumerate(((key_ref, keys), (weight_ref, weights), (coul_ref, coul)))
    ]
    barrier = pltpu.get_barrier_semaphore()

    def greet(to):
        pl.semaphore_signal(barrier, inc=1, device_id=to, device_id_type=pl.DeviceIdType.MESH)

    for to in (device["x"], device["y"], device["z"], sibling):
        greet(to)

    @pl.when(inner == 1)
    def _():
        greet(device["m"])

    for copy in small:
        copy.start()

    @pl.when(ga == 0)
    def _():
        base_local().start()

    pl.semaphore_wait(barrier, 4 + inner)

    @pl.when(ga == 0)
    def _():
        base_copy().start()

    def prepare(k):
        column = jnp.broadcast_to(coef[k][0:1, :], (LANES, bands)).T
        ccol[k] = column
        for j in range(COLS // LANES):
            re_at, im_at = pl.ds(j * LANES, LANES), pl.ds(COLS + j * LANES, LANES)
            a, b = slab[k, 0, :, re_at], slab[k, 1, :, re_at]
            total = jnp.sum(column * (2.0 - a * a - b * b), 0, keepdims=True)
            cdef[k, :, re_at] = jnp.broadcast_to(0.5 * total, (8, LANES))
            cdef[k, :, im_at] = jnp.zeros((8, LANES), jnp.float32)
            for level, (sa, sb) in enumerate(zip(split(column * a), split(column * b))):
                right[k, level, :bands, re_at] = sa
                right[k, level, bands:, re_at] = sb
                right[k, level, :bands, im_at] = sb
                right[k, level, bands:, im_at] = -sa

    def prepare_own():
        for copy in small:
            copy.wait()
        occ = (keys[...] < fermi_ref[0]).astype(jnp.float32)
        coef[0] = jnp.broadcast_to((0.5 - occ) * weights[...], coef.shape[1:])
        for t in range(CHUNKS * tiles):
            at = pl.multiple_of(ga * half + me * rows_dev + t * LANES, LANES)
            rowc[t] = jnp.broadcast_to(coul[0:1, pl.ds(at, LANES)], (LANES, LANES)).T

        @pl.when(ga == 0)
        def _():
            base_local().wait()
            base_copy().wait_send()

        @pl.when(ga == 1)
        def _():
            base_copy().wait_recv()

        prepare(0)

    def dots(slot, names):
        for i, name in enumerate(names):
            blk = block(*name)
            own_copy(*name).wait()
            m_copy(*name).wait_recv()
            for t in range(tiles):
                lanes = pl.ds(t * LANES, LANES)
                rows = pl.ds(i * width + t * LANES, LANES)
                total = jnp.zeros((1, LANES), jnp.float32)
                for ref, k, at in ((own, 0, 0), (got, slot, 2 * bands)):
                    a, b = ref[blk, 0, :, lanes], ref[blk, 1, :, lanes]
                    total += jnp.sum(ccol[k] * (2.0 - a * a - b * b), 0, keepdims=True)
                    for level, (sa, sb) in enumerate(zip(split(a.T), split(b.T))):
                        left[level, rows, at : at + bands] = sa
                        left[level, rows, at + bands : at + 2 * bands] = sb
                rdef[rows, :] = jnp.broadcast_to(0.5 * total, (LANES, LANES)).T

        step = 2 * LANES

        def product(n, _):
            at = pl.ds(pl.multiple_of(n * step, step), step)
            acc = None
            for level, other in ((0, 0), (1, 0), (0, 1)):
                for k, k_at in ((0, 0), (slot, 2 * bands)):
                    term = jnp.dot(
                        left[level, :, k_at : k_at + 2 * bands],
                        right[k, other, :, at],
                        preferred_element_type=jnp.float32,
                    )
                    acc = term if acc is None else acc + term
            keep = jnp.where(n * step < COLS, 1.0, 0.0)
            extra = rdef[...] * keep
            acc = acc + jnp.concatenate([extra, extra], 1)
            acc = acc + (cdef[0, 0:1, at] + cdef[slot, 0:1, at])
            for i, name in enumerate(names):
                part[block(*name), :, at] = acc[i * width : (i + 1) * width]
            return 0

        lax.fori_loop(0, 2 * COLS // step, product, 0)

    group = 2 * COLS // LANES

    def out_copy(c):
        rows = pl.ds(c * width * group, width * group)
        return pltpu.make_async_copy(done.at[rows], out_ref.at[rows], out_sem.at[c])

    def finish(c, one, two):
        for t in range(tiles):
            rows = pl.ds(t * LANES, LANES)
            at = pl.ds(c * width + t * LANES, LANES)
            wide = jnp.concatenate([rowc[c * tiles + t]] * (COLS // LANES), 1)
            weight = jnp.sqrt(wide * coul[0:1, :COLS])
            for p in range(2):
                cols = pl.ds(p * COLS, COLS)
                value = weight * (one[rows, cols] + two[rows, cols])
                for j in range(COLS // LANES):
                    spot = (c * width + t * LANES) * group + 2 * j + p
                    done[pl.ds(spot, LANES, stride=group), :] = value[:, j * LANES : (j + 1) * LANES]
        out_copy(c).start()

    flying = {}

    def only(cls, action):
        if cls == "B":
            action()
        else:
            pl.when(inner == (1 if cls == "I" else 0))(action)

    def wait_sent(copies):
        for make in copies:
            make().wait_send()

    def send(cls, link, *copies):
        entry = list(copies)
        waits = {}
        for c in "OI" if cls == "B" else cls:
            queue = flying.setdefault((c, link), [])
            if len(queue) >= DEPTH:
                waits[c] = queue.pop(0)
            queue.append(entry)
        if len(waits) == 2 and waits["O"] is waits["I"]:
            wait_sent(waits["O"])
            waits = {}
        for c, copies in waits.items():
            only(c, functools.partial(wait_sent, copies))

        def start():
            for make in entry:
                make().start()

        only(cls, start)

    def add(cls, copy, blk, ref, k):
        def action():
            copy().wait_recv()
            part[blk] += ref[k]

        only(cls, action)

    def do(f, *args):
        return functools.partial(f, *args)

    loads = [e[1:] for e in STEPS if e[0] == "m"]
    for e in STEPS:
        kind, rest = e[0], e[1:]
        if kind == "prep" and rest[0] == "o":
            for name in loads:
                own_copy(*name).start()
            prepare_own()
        elif kind == "slab":
            send("B", rest[0], do(slab_copy, *rest), do(coef_copy, *rest))
        elif kind == "fwd":
            slab_copy(*rest).wait_recv()
            slab_forward(*rest).start()
        elif kind == "prep":
            slab_forward(*rest).wait()
            coef_copy(*rest).wait_recv()
            prepare(SLOT[rest[0]])
        elif kind == "m":
            send("B", first_link(rest), do(m_copy, *rest))
        elif kind == "dot" and len(rest) == 3 and rest[0] < 2:
            dots(SLOT[NEAR[rest][0]], [rest + (i,) for i in range(2)])
        elif kind == "dot":
            c, k, j = rest
            dots(SLOT["z"], [(c, k, 2 * j + i) for i in range(2)])
        elif kind == "s2":
            send("B", s2_of(rest)[0], do(s2_copy, rest))
        elif kind == "a2":
            _, k, _, blk = s2_of(rest)
            add("B", do(s2_copy, rest), blk, got2, k)
        elif kind == "s3":
            send("B", FAR[rest[1]][1], do(s3_copy, *rest))
        elif kind == "a3":
            add("B", do(s3_copy, *rest), block(*rest, 0), got3, rest[1])
        elif kind == "osend":
            c, o, s = rest
            slot = end_slot(c, 1 - o, s)
            send("O", "z", do(line_copy, part.at[block(*rest, 0)], slot, "z"))
        elif kind == "iadd":
            slot = end_slot(*rest)
            add("I", do(line_copy, line.at[slot], slot, "z"), block(*rest, 0), line, slot)
        elif kind == "imid":
            c, o, s = rest
            send("I", "m", do(line_copy, part.at[block(*rest, 0)], mid_slot(c, o), "m"))
        elif kind == "imadd":
            slot = mid_slot(rest[0], 1)
            add("I", do(line_copy, line.at[slot], slot, "m"), block(*rest, 0), line, slot)
        elif kind == "iout":
            (c,) = rest
            send("I", "z", do(line_copy, part.at[block(c, 1, 0, 0)], c * LINE_SLOTS, "z"))
        elif kind in ("ifin", "ofin"):
            (c,) = rest
            slot, link = (mid_slot(c, 0), "m") if kind == "ifin" else (c * LINE_SLOTS, "z")

            def action(c=c, slot=slot, link=link):
                line_copy(line.at[slot], slot, link).wait_recv()
                finish(c, part.at[block(c, 0, 0, 0)], line.at[slot])

            only("I" if kind == "ifin" else "O", action)
        elif kind == "imid2":
            (k,) = rest
            send("I", "m", do(line_copy, part.at[block(2, k, 0)], far_line + 1 + k, "m"))
        elif kind == "osend2":
            send("O", "z", do(line_copy, part.at[block(2, 1, 0)], far_line, "z"))
        elif kind == "iout2":
            def arrived():
                line_copy(line.at[far_line + 2], far_line + 2, "m").wait_recv()

            only("I", arrived)
            send("I", "z", do(line_copy, line.at[far_line + 2], far_line, "z"))
        elif kind == "ifin2":
            def action():
                line_copy(line.at[far_line + 1], far_line + 1, "m").wait_recv()
                line_copy(line.at[far_line], far_line, "z").wait_recv()
                finish(2, line.at[far_line], line.at[far_line + 1])

            only("I", action)
        elif kind == "ofin2":
            def action():
                line_copy(line.at[far_line], far_line, "z").wait_recv()
                finish(2, part.at[block(2, 0, 0)], line.at[far_line])

            only("O", action)

    for c in "OI":
        def drain(c=c):
            for (cls, _), queue in flying.items():
                for copies in queue if cls == c else ():
                    wait_sent(copies)

        only(c, drain)
    for c in range(CHUNKS):
        out_copy(c).wait()


def spread(factor, in_ref, out_ref, held, sems):
    pieces = held.shape[0]
    rows = held.shape[1]

    def copy(way, i):
        at = pl.ds(i * rows, rows)
        if way == 0:
            return pltpu.make_async_copy(in_ref.at[at], held.at[i], sems.at[0, i])
        return pltpu.make_async_copy(held.at[i], out_ref.at[at], sems.at[1, i])

    for i in range(pieces):
        copy(0, i).start()
    for i in range(pieces):
        copy(0, i).wait()
        held[i] = held[i] * factor
        copy(1, i).start()
    for i in range(pieces):
        copy(1, i).wait()


def body_fast(matrix_elements, band_index, occupied, band_weight, coulomb):
    bands = matrix_elements.shape[1]
    half = matrix_elements.shape[2]
    n_band = lax.axis_size("band")
    rows_dev = half // n_band
    width = rows_dev // CHUNKS
    factor = 1.0 / math.sqrt(bands * n_band)
    f32 = jnp.float32
    hbm = pl.BlockSpec(memory_space=pl.ANY)
    blocks = 8 * CHUNKS
    near_streams = 2 * len(LINE)
    dma = pltpu.SemaphoreType.DMA
    total = pl.pallas_call(
        functools.partial(kernel, rows_dev),
        out_shape=jax.ShapeDtypeStruct((rows_dev * 2 * COLS // LANES, LANES), f32),
        in_specs=[hbm, hbm, pl.BlockSpec(memory_space=pltpu.SMEM), hbm, hbm],
        out_specs=hbm,
        scratch_shapes=[
            pltpu.VMEM((rows_dev * 2 * COLS // LANES, LANES), f32),
            pltpu.VMEM((1, bands), jnp.int32),
            pltpu.VMEM((1, bands), f32),
            pltpu.VMEM((1, coulomb.shape[0]), f32),
            pltpu.VMEM((rows_dev // LANES, LANES, LANES), f32),
            pltpu.VMEM((4, 2, bands, COLS), f32),
            pltpu.VMEM((4, 8, bands), f32),
            pltpu.VMEM((4, bands, LANES), f32),
            pltpu.VMEM((4, 2, 2 * bands, 2 * COLS), jnp.bfloat16),
            pltpu.VMEM((4, 8, 2 * COLS), f32),
            pltpu.VMEM((blocks, 2, bands, width), f32),
            pltpu.VMEM((blocks, 2, bands, width), f32),
            pltpu.VMEM((2, 2 * width, 4 * bands), jnp.bfloat16),
            pltpu.VMEM((2 * width, LANES), f32),
            pltpu.VMEM((blocks, width, 2 * COLS), f32),
            pltpu.VMEM((near_streams + 4, width, 2 * COLS), f32),
            pltpu.VMEM((2, width, 2 * COLS), f32),
            pltpu.VMEM((2 * LINE_SLOTS + 3, width, 2 * COLS), f32),
            dma((3,)), dma((2, 2)), dma((2, 3)), dma((2, 3)), dma((2, 3)), dma((blocks,)),
            dma((2, blocks)), dma((2, near_streams + 4)), dma((2, 2)), dma((2, 2 * LINE_SLOTS + 3)),
            dma((CHUNKS,)),
        ],
        compiler_params=pltpu.CompilerParams(
            collective_id=0, has_side_effects=True, vmem_limit_bytes=VMEM_BYTES
        ),
        name="reduce_sums",
    )(
        matrix_elements, band_index.reshape(1, bands), occupied, band_weight.reshape(1, bands),
        coulomb.reshape(1, coulomb.shape[0]),
    )
    total = pl.pallas_call(
        functools.partial(spread, factor),
        out_shape=jax.ShapeDtypeStruct(total.shape, f32),
        in_specs=[hbm],
        out_specs=hbm,
        scratch_shapes=[pltpu.VMEM((PIECES, total.shape[0] // PIECES, LANES), f32), dma((2, PIECES))],
        name="spread",
    )(total)
    parts = total.reshape(rows_dev, COLS // LANES, 2, LANES)
    return parts.transpose(0, 2, 1, 3).reshape(rows_dev, 2, COLS)


def solution(mesh):
    n_band, n_ga = mesh.shape["band"], mesh.shape["ga"]

    def body(matrix_elements, *rest):
        rows_dev = matrix_elements.shape[2] // n_band
        aligned = rows_dev % (CHUNKS * LANES) == 0 and matrix_elements.shape[1] % LANES == 0
        if n_band == 1 << len(LINE) and n_ga == 2 and aligned:
            return body_fast(matrix_elements, *rest)
        return body_plain(matrix_elements, *rest)

    return jax.shard_map(
        body,
        mesh=mesh,
        in_specs=(P(None, "band", "ga"), P("band"), P(), P("band"), P()),
        out_specs=P(("ga", "band"), None, None),
        check_vma=False,
    )
```

```python
import functools
import math

import jax
import jax.numpy as jnp
from jax import lax
from jax.experimental import pallas as pl
from jax.experimental.pallas import tpu as pltpu
from jax.sharding import PartitionSpec as P

COLS = 512
LANES = 128
CHUNKS = 3
DEPTH = 2
VMEM_BYTES = 58 * 1024 * 1024

X_BIT, Y_BIT, Z_BIT, S_BIT = 0, 1, 2, 3
BIT = {"x": X_BIT, "y": Y_BIT, "z": Z_BIT}
SLOT = {"x": 1, "y": 2, "z": 3}
LINE = ((0, 1), (1, 1), (1, 0), (0, 0))
LINE_SLOT = {(0, 1): 0, (1, 1): 1, (0, 0): 2}
LINE_SLOTS = 5
NEAR = {
    (0, 0, 1): "xy", (0, 1, 1): "yx", (0, 1, 0): "xy", (0, 0, 0): "yx", (1, 0, 1): "yx", (1, 1, 1): "xy",
    (1, 1, 0): "yx", (1, 0, 0): "xy",
}
FAR = {0: "xy", 1: "yx"}
STEPS = (
    ("m", 2, 1, 1), ("m", 0, 0, 1, 0), ("m", 2, 1, 3), ("m", 0, 1, 1, 0), ("m", 1, 0, 1, 0), ("m", 1, 1, 1, 0),
    ("prep", "o"), ("slab", "z"), ("slab", "x"), ("slab", "y"), ("m", 2, 1, 2), ("m", 0, 1, 0, 1), ("m", 0, 1, 1, 1),
    ("m", 2, 0, 3), ("m", 0, 0, 1, 1), ("m", 1, 0, 1, 1), ("fwd", "z"), ("fwd", "x"), ("fwd", "y"), ("prep", "z"),
    ("prep", "x"), ("prep", "y"), ("m", 2, 1, 0), ("m", 1, 0, 0, 1), ("m", 1, 1, 0, 1), ("dot", 2, 1, 1),
    ("dot", 0, 1, 1), ("s2", 0, 1, 1), ("s2", 2, 1, 1), ("m", 2, 0, 2), ("dot", 0, 0, 1), ("dot", 1, 0, 1),
    ("s2", 0, 0, 1), ("s2", 1, 0, 1), ("dot", 2, 1, 0), ("m", 2, 0, 0), ("m", 2, 0, 1), ("dot", 2, 0, 1),
    ("m", 1, 1, 1, 1), ("s2", 2, 1, 0), ("a2", 0, 1, 1), ("osend", 0, 1, 1), ("a2", 2, 1, 1), ("dot", 2, 0, 0),
    ("s3", 2, 1), ("m", 1, 1, 0, 0), ("a2", 1, 0, 1), ("osend", 1, 0, 1), ("a2", 0, 0, 1), ("osend", 0, 0, 1),
    ("m", 0, 1, 0, 0), ("iadd", 0, 0, 1), ("imid", 0, 0, 1), ("dot", 1, 1, 1), ("s2", 1, 1, 1), ("a2", 2, 1, 0),
    ("s2", 2, 0, 1), ("m", 0, 0, 0, 0), ("a3", 2, 1), ("osend2",), ("imid2", 1), ("dot", 1, 1, 0), ("s2", 1, 1, 0),
    ("dot", 0, 1, 0), ("s2", 0, 1, 0), ("iadd", 0, 1, 1), ("imid", 0, 1, 1), ("a2", 1, 1, 1), ("iadd", 1, 1, 1),
    ("imid", 1, 1, 1), ("osend", 1, 1, 1), ("iout2",), ("m", 1, 0, 0, 0), ("m", 0, 0, 0, 1), ("a2", 2, 0, 1),
    ("s2", 2, 0, 0), ("s3", 2, 0), ("a2", 1, 1, 0), ("osend", 1, 1, 0), ("a2", 0, 1, 0), ("imadd", 0, 1, 0),
    ("iout", 0), ("osend", 0, 1, 0), ("iadd", 1, 0, 1), ("imid", 1, 0, 1), ("dot", 1, 0, 0), ("s2", 1, 0, 0),
    ("imadd", 1, 1, 0), ("iout", 1), ("dot", 0, 0, 0), ("s2", 0, 0, 0), ("a2", 2, 0, 0), ("a3", 2, 0), ("imid2", 0),
    ("ofin2",), ("a2", 0, 0, 0), ("ofin", 0), ("a2", 1, 0, 0), ("iadd", 1, 0, 0), ("ifin", 1), ("ofin", 1),
    ("iadd", 0, 0, 0), ("ifin", 0), ("ifin2",),
)


def contract(left, right):
    return lax.dot_general(
        left,
        right,
        (((0,), (0,)), ((), ())),
        precision=lax.Precision.HIGH,
        preferred_element_type=jnp.float32,
    )


def right_side(slab):
    return jnp.concatenate(
        [jnp.concatenate([slab[0], slab[1]], 1), jnp.concatenate([slab[1], -slab[0]], 1)], 0
    )


def defects(coef, block):
    return jnp.sum(coef[:, None] * (2.0 - block[0] * block[0] - block[1] * block[1]), 0)


def body_plain(matrix_elements, band_index, occupied, band_weight, coulomb):
    bands_dev = matrix_elements.shape[1]
    half = matrix_elements.shape[2]
    n_band = lax.axis_size("band")
    n_bits = n_band.bit_length() - 1
    rows_dev = half // n_band
    n_ga = lax.axis_size("ga")
    chunks = 3 if rows_dev % 3 == 0 else 1
    width = rows_dev // chunks
    factor = 1.0 / math.sqrt(bands_dev * n_band)
    band_pos = lax.axis_index("band")
    ga_pos = lax.axis_index("ga")
    bits = list(range(n_bits - 1))
    top = n_band // 2
    firsts = [b % len(bits) for b in range(chunks)]
    streams = [(c, p) for p in range(2) for c in range(chunks)]
    orders = {}
    for c, p in streams:
        rest = bits[firsts[c] + 1 :] + bits[: firsts[c]]
        orders[c, p] = rest[p:] + rest[:p]

    def swap(x, bit):
        return lax.ppermute(x, "band", [(i, i ^ (1 << bit)) for i in range(n_band)])

    def mine(bit):
        return (band_pos >> bit) & 1

    def pick(x, c, p, which):
        bit = firsts[c]
        parts = []
        for d in range(p * top, (p + 1) * top):
            if not (d >> bit) & 1:
                low = d * rows_dev + c * width
                high = (d | (1 << bit)) * rows_dev + c * width
                parts.append(
                    jnp.where(which == 1, x[..., high : high + width], x[..., low : low + width])
                )
        return jnp.concatenate(parts, -1)

    there = {
        (c, p): swap(pick(matrix_elements, c, p, 1 - mine(firsts[c])), firsts[c])
        for c, p in streams
    }

    occ = (band_index < occupied[0]).astype(jnp.float32)
    coef = (0.5 - occ) * band_weight
    first = matrix_elements[:, :, :COLS]
    moved = lax.ppermute(first, "ga", [(0, g) for g in range(1, n_ga)][:1])
    slab = jnp.where(ga_pos == 0, first, moved)
    scaled = coef[None, :, None] * slab
    right = right_side(scaled)
    rights = [right_side(swap(scaled, bit)) for bit in firsts]
    row_def = defects(coef, matrix_elements)
    col_def = defects(coef, slab)

    sums, left = {}, {}
    for c, p in streams:
        bit = firsts[c]
        rows_here = pick(row_def, c, p, mine(bit))
        send = jnp.concatenate([pick(row_def, c, p, 1 - mine(bit)), col_def])
        got = swap(send, bit)
        count = rows_here.shape[0]
        rows_sum = rows_here + got[:count]
        cols_sum = col_def + got[count:]
        here = pick(matrix_elements, c, p, mine(bit))
        part = contract(here.reshape(2 * bands_dev, count), right)
        part = part + contract(there[c, p].reshape(2 * bands_dev, count), rights[c])
        extra = 0.5 * (rows_sum[:, None] + cols_sum[None, :])
        part = part + jnp.concatenate([extra, jnp.zeros_like(extra)], 1)
        sums[c, p] = part.reshape((2,) * (n_bits - 2) + (width, 2 * COLS))
        left[c, p] = [b for b in reversed(bits) if b != bit]

    for step in range(n_bits - 2):
        sent = {}
        for k in streams:
            bit = orders[k][step]
            send = lax.dynamic_index_in_dim(
                sums[k], 1 - mine(bit), left[k].index(bit), keepdims=False
            )
            sent[k] = swap(send, bit)
        for k in streams:
            bit = orders[k][step]
            keep = lax.dynamic_index_in_dim(sums[k], mine(bit), left[k].index(bit), keepdims=False)
            sums[k] = keep + sent[k]
            left[k].remove(bit)

    upper = mine(n_bits - 1) == 1
    last = [swap(jnp.where(upper, sums[c, 0], sums[c, 1]), n_bits - 1) for c in range(chunks)]
    done = [jnp.where(upper, sums[c, 1], sums[c, 0]) + last[c] for c in range(chunks)]
    total = jnp.concatenate(done, 0)
    row_coul = lax.dynamic_slice_in_dim(coulomb, ga_pos * half + band_pos * rows_dev, rows_dev, 0)
    weight = factor * jnp.sqrt(row_coul[:, None] * coulomb[None, :COLS])
    return jnp.stack([weight * total[:, :COLS], weight * total[:, COLS:]], 1)


def split(value):
    high = value.astype(jnp.bfloat16)
    return high, (value - high.astype(jnp.float32)).astype(jnp.bfloat16)


def kernel(
    rows_dev, factor, m_ref, key_ref, fermi_ref, weight_ref, coul_ref, out_ref,
    keys, weights, coul, rowc, slab, coef, ccol, right, cdef, own, got, left, rdef, part, got2, got3, line,
    small_sem, base_sem, slab_sem, fwd_sem, coef_sem, own_sem, m_sem, s2_sem, s3_sem, line_sem,
):
    bands, half = m_ref.shape[1], m_ref.shape[2]
    width = rows_dev // CHUNKS
    tiles = width // LANES
    me = lax.axis_index("band")
    ga = lax.axis_index("ga")
    mine = [lax.rem(me // (1 << b), 2) for b in range(4)]

    def flip(bit, by):
        return bit + by - 2 * bit * by

    inner = flip(mine[Z_BIT], mine[S_BIT])

    def across(*bits):
        return {"band": me + sum((1 - 2 * mine[b]) * (1 << b) for b in bits)}

    device = {"x": across(X_BIT), "y": across(Y_BIT), "z": across(Z_BIT), "m": across(Z_BIT, S_BIT)}
    sibling = {"ga": 1 - ga}

    def rows_of(c, flips):
        dest = sum(flip(mine[b], flips[b]) * (1 << b) for b in range(4))
        return pl.ds(pl.multiple_of(dest * rows_dev + c * width, LANES), width)

    far_base = 8 * len(LINE) // 2

    def near(c, o, s):
        return c * len(LINE) + LINE.index((o, s))

    def block(*name):
        if len(name) == 4:
            return 2 * near(*name[:3]) + name[3]
        return far_base + 4 * name[1] + name[2]

    def m_rows(sent, *name):
        if len(name) == 4:
            c, o, s, i = name
            first, second = NEAR[c, o, s]
            return rows_of(c, {BIT[first]: sent, BIT[second]: i, Z_BIT: o ^ s, S_BIT: s})
        c, k, i = name
        second, third = FAR[k]
        o, s = (1 - k, 1 - inner) if sent else (k, inner)
        return rows_of(c, {BIT[second]: i // 2, BIT[third]: i % 2, Z_BIT: flip(s, o), S_BIT: s})

    def first_link(name):
        return NEAR[name[:3]][0] if len(name) == 4 else "z"

    def remote(src, dst, sems, k, to):
        return pltpu.make_async_remote_copy(
            src_ref=src, dst_ref=dst, send_sem=sems.at[0, k], recv_sem=sems.at[1, k],
            device_id=to, device_id_type=pl.DeviceIdType.MESH,
        )

    def base_copy():
        return remote(m_ref.at[:, :, pl.ds(0, COLS)], slab.at[0], base_sem, 0, sibling)

    def base_local():
        return pltpu.make_async_copy(m_ref.at[:, :, pl.ds(0, COLS)], slab.at[0], base_sem.at[0, 1])

    def slab_copy(b):
        k = SLOT[b]
        return remote(slab.at[0, ga], slab.at[k, ga], slab_sem, k - 1, device[b])

    def slab_forward(b):
        k = SLOT[b]
        return remote(slab.at[k, ga], slab.at[k, ga], fwd_sem, k - 1, sibling)

    def coef_copy(b):
        k = SLOT[b]
        return remote(coef.at[0], coef.at[k], coef_sem, k - 1, device[b])

    def m_copy(*name):
        k = block(*name)
        return remote(m_ref.at[:, :, m_rows(1, *name)], got.at[k], m_sem, k, device[first_link(name)])

    def own_copy(*name):
        k = block(*name)
        return pltpu.make_async_copy(m_ref.at[:, :, m_rows(0, *name)], own.at[k], own_sem.at[k])

    def s2_of(name):
        if name[0] < 2:
            k = near(*name)
            return NEAR[name][1], k, block(*name, 1), block(*name, 0)
        c, k, r = name
        return FAR[k][0], far_base // 2 + 2 * k + r, block(c, k, 2 + r), block(c, k, r)

    def s2_copy(name):
        link, k, sent, _ = s2_of(name)
        return remote(part.at[sent], got2.at[k], s2_sem, k, device[link])

    def s3_copy(c, k):
        return remote(part.at[block(c, k, 1)], got3.at[k], s3_sem, k, device[FAR[k][1]])

    far_line = 2 * LINE_SLOTS

    def line_copy(src, slot, link):
        return remote(src, line.at[slot], line_sem, slot, device[link])

    def end_slot(c, o, s):
        return c * LINE_SLOTS + LINE_SLOT[o, s]

    def mid_slot(c, o):
        return c * LINE_SLOTS + 3 + o

    small = [
        pltpu.make_async_copy(src, dst, small_sem.at[i])
        for i, (src, dst) in enumerate(((key_ref, keys), (weight_ref, weights), (coul_ref, coul)))
    ]
    barrier = pltpu.get_barrier_semaphore()

    def greet(to):
        pl.semaphore_signal(barrier, inc=1, device_id=to, device_id_type=pl.DeviceIdType.MESH)

    for to in (device["x"], device["y"], device["z"], sibling):
        greet(to)

    @pl.when(inner == 1)
    def _():
        greet(device["m"])

    for copy in small:
        copy.start()

    @pl.when(ga == 0)
    def _():
        base_local().start()

    pl.semaphore_wait(barrier, 4 + inner)

    @pl.when(ga == 0)
    def _():
        base_copy().start()

    def prepare(k):
        column = jnp.broadcast_to(coef[k][0:1, :], (LANES, bands)).T
        ccol[k] = column
        for j in range(COLS // LANES):
            re_at, im_at = pl.ds(j * LANES, LANES), pl.ds(COLS + j * LANES, LANES)
            a, b = slab[k, 0, :, re_at], slab[k, 1, :, re_at]
            total = jnp.sum(column * (2.0 - a * a - b * b), 0, keepdims=True)
            cdef[k, :, re_at] = jnp.broadcast_to(0.5 * total, (8, LANES))
            cdef[k, :, im_at] = jnp.zeros((8, LANES), jnp.float32)
            for level, (sa, sb) in enumerate(zip(split(column * a), split(column * b))):
                right[k, level, :bands, re_at] = sa
                right[k, level, bands:, re_at] = sb
                right[k, level, :bands, im_at] = sb
                right[k, level, bands:, im_at] = -sa

    def prepare_own():
        for copy in small:
            copy.wait()
        occ = (keys[...] < fermi_ref[0]).astype(jnp.float32)
        coef[0] = jnp.broadcast_to((0.5 - occ) * weights[...], coef.shape[1:])
        for t in range(CHUNKS * tiles):
            at = pl.multiple_of(ga * half + me * rows_dev + t * LANES, LANES)
            rowc[t] = jnp.broadcast_to(coul[0:1, pl.ds(at, LANES)], (LANES, LANES)).T

        @pl.when(ga == 0)
        def _():
            base_local().wait()
            base_copy().wait_send()

        @pl.when(ga == 1)
        def _():
            base_copy().wait_recv()

        prepare(0)

    def dots(slot, names):
        for i, name in enumerate(names):
            blk = block(*name)
            own_copy(*name).wait()
            m_copy(*name).wait_recv()
            for t in range(tiles):
                lanes = pl.ds(t * LANES, LANES)
                rows = pl.ds(i * width + t * LANES, LANES)
                total = jnp.zeros((1, LANES), jnp.float32)
                for ref, k, at in ((own, 0, 0), (got, slot, 2 * bands)):
                    a, b = ref[blk, 0, :, lanes], ref[blk, 1, :, lanes]
                    total += jnp.sum(ccol[k] * (2.0 - a * a - b * b), 0, keepdims=True)
                    for level, (sa, sb) in enumerate(zip(split(a.T), split(b.T))):
                        left[level, rows, at : at + bands] = sa
                        left[level, rows, at + bands : at + 2 * bands] = sb
                rdef[rows, :] = jnp.broadcast_to(0.5 * total, (LANES, LANES)).T

        step = 2 * LANES

        def product(n, _):
            at = pl.ds(pl.multiple_of(n * step, step), step)
            acc = None
            for level, other in ((0, 0), (1, 0), (0, 1)):
                for k, k_at in ((0, 0), (slot, 2 * bands)):
                    term = jnp.dot(
                        left[level, :, k_at : k_at + 2 * bands],
                        right[k, other, :, at],
                        preferred_element_type=jnp.float32,
                    )
                    acc = term if acc is None else acc + term
            keep = jnp.where(n * step < COLS, 1.0, 0.0)
            extra = rdef[...] * keep
            acc = acc + jnp.concatenate([extra, extra], 1)
            acc = acc + (cdef[0, 0:1, at] + cdef[slot, 0:1, at])
            for i, name in enumerate(names):
                part[block(*name), :, at] = acc[i * width : (i + 1) * width]
            return 0

        lax.fori_loop(0, 2 * COLS // step, product, 0)

    group = 2 * COLS // LANES

    def finish(c, one, two):
        for t in range(tiles):
            rows = pl.ds(t * LANES, LANES)
            at = pl.ds(c * width + t * LANES, LANES)
            wide = jnp.concatenate([rowc[c * tiles + t]] * (COLS // LANES), 1)
            weight = factor * jnp.sqrt(wide * coul[0:1, :COLS])
            for p in range(2):
                cols = pl.ds(p * COLS, COLS)
                value = weight * (one[rows, cols] + two[rows, cols])
                for j in range(COLS // LANES):
                    spot = (c * width + t * LANES) * group + 2 * j + p
                    out_ref[pl.ds(spot, LANES, stride=group), :] = value[:, j * LANES : (j + 1) * LANES]

    flying = {}

    def only(cls, action):
        if cls == "B":
            action()
        else:
            pl.when(inner == (1 if cls == "I" else 0))(action)

    def wait_sent(copies):
        for make in copies:
            make().wait_send()

    def send(cls, link, *copies):
        entry = list(copies)
        waits = {}
        for c in "OI" if cls == "B" else cls:
            queue = flying.setdefault((c, link), [])
            if len(queue) >= DEPTH:
                waits[c] = queue.pop(0)
            queue.append(entry)
        if len(waits) == 2 and waits["O"] is waits["I"]:
            wait_sent(waits["O"])
            waits = {}
        for c, copies in waits.items():
            only(c, functools.partial(wait_sent, copies))

        def start():
            for make in entry:
                make().start()

        only(cls, start)

    def add(cls, copy, blk, ref, k):
        def action():
            copy().wait_recv()
            part[blk] += ref[k]

        only(cls, action)

    def do(f, *args):
        return functools.partial(f, *args)

    loads = [e[1:] for e in STEPS if e[0] == "m"]
    for e in STEPS:
        kind, rest = e[0], e[1:]
        if kind == "prep" and rest[0] == "o":
            for name in loads:
                own_copy(*name).start()
            prepare_own()
        elif kind == "slab":
            send("B", rest[0], do(slab_copy, *rest), do(coef_copy, *rest))
        elif kind == "fwd":
            slab_copy(*rest).wait_recv()
            slab_forward(*rest).start()
        elif kind == "prep":
            slab_forward(*rest).wait()
            coef_copy(*rest).wait_recv()
            prepare(SLOT[rest[0]])
        elif kind == "m":
            send("B", first_link(rest), do(m_copy, *rest))
        elif kind == "dot" and len(rest) == 3 and rest[0] < 2:
            dots(SLOT[NEAR[rest][0]], [rest + (i,) for i in range(2)])
        elif kind == "dot":
            c, k, j = rest
            dots(SLOT["z"], [(c, k, 2 * j + i) for i in range(2)])
        elif kind == "s2":
            send("B", s2_of(rest)[0], do(s2_copy, rest))
        elif kind == "a2":
            _, k, _, blk = s2_of(rest)
            add("B", do(s2_copy, rest), blk, got2, k)
        elif kind == "s3":
            send("B", FAR[rest[1]][1], do(s3_copy, *rest))
        elif kind == "a3":
            add("B", do(s3_copy, *rest), block(*rest, 0), got3, rest[1])
        elif kind == "osend":
            c, o, s = rest
            slot = end_slot(c, 1 - o, s)
            send("O", "z", do(line_copy, part.at[block(*rest, 0)], slot, "z"))
        elif kind == "iadd":
            slot = end_slot(*rest)
            add("I", do(line_copy, line.at[slot], slot, "z"), block(*rest, 0), line, slot)
        elif kind == "imid":
            c, o, s = rest
            send("I", "m", do(line_copy, part.at[block(*rest, 0)], mid_slot(c, o), "m"))
        elif kind == "imadd":
            slot = mid_slot(rest[0], 1)
            add("I", do(line_copy, line.at[slot], slot, "m"), block(*rest, 0), line, slot)
        elif kind == "iout":
            (c,) = rest
            send("I", "z", do(line_copy, part.at[block(c, 1, 0, 0)], c * LINE_SLOTS, "z"))
        elif kind in ("ifin", "ofin"):
            (c,) = rest
            slot, link = (mid_slot(c, 0), "m") if kind == "ifin" else (c * LINE_SLOTS, "z")

            def action(c=c, slot=slot, link=link):
                line_copy(line.at[slot], slot, link).wait_recv()
                finish(c, part.at[block(c, 0, 0, 0)], line.at[slot])

            only("I" if kind == "ifin" else "O", action)
        elif kind == "imid2":
            (k,) = rest
            send("I", "m", do(line_copy, part.at[block(2, k, 0)], far_line + 1 + k, "m"))
        elif kind == "osend2":
            send("O", "z", do(line_copy, part.at[block(2, 1, 0)], far_line, "z"))
        elif kind == "iout2":
            def arrived():
                line_copy(line.at[far_line + 2], far_line + 2, "m").wait_recv()

            only("I", arrived)
            send("I", "z", do(line_copy, line.at[far_line + 2], far_line, "z"))
        elif kind == "ifin2":
            def action():
                line_copy(line.at[far_line + 1], far_line + 1, "m").wait_recv()
                line_copy(line.at[far_line], far_line, "z").wait_recv()
                finish(2, line.at[far_line], line.at[far_line + 1])

            only("I", action)
        elif kind == "ofin2":
            def action():
                line_copy(line.at[far_line], far_line, "z").wait_recv()
                finish(2, part.at[block(2, 0, 0)], line.at[far_line])

            only("O", action)

    for c in "OI":
        def drain(c=c):
            for (cls, _), queue in flying.items():
                for copies in queue if cls == c else ():
                    wait_sent(copies)

        only(c, drain)


def body_fast(matrix_elements, band_index, occupied, band_weight, coulomb):
    bands = matrix_elements.shape[1]
    half = matrix_elements.shape[2]
    n_band = lax.axis_size("band")
    rows_dev = half // n_band
    width = rows_dev // CHUNKS
    factor = 1.0 / math.sqrt(bands * n_band)
    f32 = jnp.float32
    hbm = pl.BlockSpec(memory_space=pl.ANY)
    blocks = 8 * CHUNKS
    near_streams = 2 * len(LINE)
    dma = pltpu.SemaphoreType.DMA
    total = pl.pallas_call(
        functools.partial(kernel, rows_dev, factor),
        out_shape=pltpu.VMEM((rows_dev * 2 * COLS // LANES, LANES), f32),
        in_specs=[hbm, hbm, pl.BlockSpec(memory_space=pltpu.SMEM), hbm, hbm],
        out_specs=pl.BlockSpec(memory_space=pltpu.VMEM),
        scratch_shapes=[
            pltpu.VMEM((1, bands), jnp.int32),
            pltpu.VMEM((1, bands), f32),
            pltpu.VMEM((1, coulomb.shape[0]), f32),
            pltpu.VMEM((rows_dev // LANES, LANES, LANES), f32),
            pltpu.VMEM((4, 2, bands, COLS), f32),
            pltpu.VMEM((4, 8, bands), f32),
            pltpu.VMEM((4, bands, LANES), f32),
            pltpu.VMEM((4, 2, 2 * bands, 2 * COLS), jnp.bfloat16),
            pltpu.VMEM((4, 8, 2 * COLS), f32),
            pltpu.VMEM((blocks, 2, bands, width), f32),
            pltpu.VMEM((blocks, 2, bands, width), f32),
            pltpu.VMEM((2, 2 * width, 4 * bands), jnp.bfloat16),
            pltpu.VMEM((2 * width, LANES), f32),
            pltpu.VMEM((blocks, width, 2 * COLS), f32),
            pltpu.VMEM((near_streams + 4, width, 2 * COLS), f32),
            pltpu.VMEM((2, width, 2 * COLS), f32),
            pltpu.VMEM((2 * LINE_SLOTS + 3, width, 2 * COLS), f32),
            dma((3,)), dma((2, 2)), dma((2, 3)), dma((2, 3)), dma((2, 3)), dma((blocks,)),
            dma((2, blocks)), dma((2, near_streams + 4)), dma((2, 2)), dma((2, 2 * LINE_SLOTS + 3)),
        ],
        compiler_params=pltpu.CompilerParams(
            collective_id=0, has_side_effects=True, vmem_limit_bytes=VMEM_BYTES
        ),
        name="reduce_sums",
    )(
        matrix_elements, band_index.reshape(1, bands), occupied, band_weight.reshape(1, bands),
        coulomb.reshape(1, coulomb.shape[0]),
    )
    parts = total.reshape(rows_dev, COLS // LANES, 2, LANES)
    return parts.transpose(0, 2, 1, 3).reshape(rows_dev, 2, COLS)


def solution(mesh):
    n_band, n_ga = mesh.shape["band"], mesh.shape["ga"]

    def body(matrix_elements, *rest):
        rows_dev = matrix_elements.shape[2] // n_band
        aligned = rows_dev % (CHUNKS * LANES) == 0 and matrix_elements.shape[1] % LANES == 0
        if n_band == 1 << len(LINE) and n_ga == 2 and aligned:
            return body_fast(matrix_elements, *rest)
        return body_plain(matrix_elements, *rest)

    return jax.shard_map(
        body,
        mesh=mesh,
        in_specs=(P(None, "band", "ga"), P("band"), P(), P("band"), P()),
        out_specs=P(("ga", "band"), None, None),
        check_vma=False,
    )
```

```python
import functools
import math

import jax
import jax.numpy as jnp
from jax import lax
from jax.experimental import pallas as pl
from jax.experimental.pallas import tpu as pltpu
from jax.sharding import PartitionSpec as P

COLS = 512
LANES = 128
CHUNKS = 3
DEPTH = 2
VMEM_BYTES = 58 * 1024 * 1024

X_BIT, Y_BIT, Z_BIT, S_BIT = 0, 1, 2, 3
BIT = {"x": X_BIT, "y": Y_BIT, "z": Z_BIT}
SLOT = {"x": 1, "y": 2, "z": 3}
LINE = ((0, 1), (1, 1), (1, 0), (0, 0))
LINE_SLOT = {(0, 1): 0, (1, 1): 1, (0, 0): 2}
LINE_SLOTS = 5
NEAR = {
    (0, 0, 1): "xy", (0, 1, 1): "yx", (0, 1, 0): "xy", (0, 0, 0): "yx", (1, 0, 1): "yx", (1, 1, 1): "xy",
    (1, 1, 0): "yx", (1, 0, 0): "xy",
}
FAR = {0: "xy", 1: "yx"}
STEPS = (
    ("m", 0, 0, 1, 0), ("m", 2, 1, 1), ("m", 0, 1, 1, 0), ("m", 0, 1, 0, 0), ("m", 0, 1, 1, 1), ("m", 2, 1, 3),
    ("prep", "o"), ("slab", "x"), ("slab", "z"), ("slab", "y"), ("m", 0, 0, 1, 1), ("m", 2, 1, 2), ("m", 1, 0, 1, 0),
    ("m", 1, 1, 1, 0), ("m", 2, 0, 2), ("m", 1, 0, 1, 1), ("fwd", "x"), ("fwd", "z"), ("fwd", "y"), ("prep", "x"),
    ("prep", "z"), ("prep", "y"), ("dot", 0, 1, 1), ("dot", 2, 1, 1), ("s2", 2, 1, 1), ("s2", 0, 1, 1),
    ("m", 2, 1, 0), ("dot", 0, 0, 1), ("s2", 0, 0, 1), ("m", 1, 1, 1, 1), ("dot", 1, 0, 1), ("m", 2, 0, 3),
    ("m", 2, 0, 0), ("dot", 2, 1, 0), ("s2", 1, 0, 1), ("m", 2, 0, 1), ("s2", 2, 1, 0), ("a2", 0, 1, 1),
    ("dot", 2, 0, 1), ("a2", 2, 1, 1), ("s3", 2, 1), ("osend", 0, 1, 1), ("dot", 1, 1, 1), ("s2", 1, 1, 1),
    ("dot", 2, 0, 0), ("a2", 0, 0, 1), ("osend", 0, 0, 1), ("m", 1, 0, 0, 1), ("a2", 1, 0, 1), ("osend", 1, 0, 1),
    ("m", 1, 1, 0, 1), ("iadd", 0, 0, 1), ("imid", 0, 0, 1), ("a2", 2, 1, 0), ("m", 0, 1, 0, 1), ("a3", 2, 1),
    ("imid2", 1), ("s2", 2, 0, 1), ("osend2",), ("m", 1, 1, 0, 0), ("iadd", 0, 1, 1), ("imid", 0, 1, 1),
    ("a2", 1, 1, 1), ("m", 1, 0, 0, 0), ("m", 0, 0, 0, 0), ("dot", 0, 1, 0), ("osend", 1, 1, 1), ("s2", 0, 1, 0),
    ("iadd", 1, 1, 1), ("dot", 1, 1, 0), ("imid", 1, 1, 1), ("iout2",), ("s2", 1, 1, 0), ("m", 0, 0, 0, 1),
    ("a2", 2, 0, 1), ("s2", 2, 0, 0), ("dot", 1, 0, 0), ("s3", 2, 0), ("a2", 0, 1, 0), ("imadd", 0, 1, 0),
    ("iout", 0), ("osend", 0, 1, 0), ("s2", 1, 0, 0), ("a2", 1, 1, 0), ("iadd", 1, 0, 1), ("osend", 1, 1, 0),
    ("imid", 1, 0, 1), ("dot", 0, 0, 0), ("s2", 0, 0, 0), ("imadd", 1, 1, 0), ("iout", 1), ("a2", 2, 0, 0),
    ("a3", 2, 0), ("imid2", 0), ("ofin2",), ("a2", 0, 0, 0), ("ofin", 0), ("a2", 1, 0, 0), ("ofin", 1),
    ("iadd", 1, 0, 0), ("ifin", 1), ("iadd", 0, 0, 0), ("ifin", 0), ("ifin2",),
)


def contract(left, right):
    return lax.dot_general(
        left,
        right,
        (((0,), (0,)), ((), ())),
        precision=lax.Precision.HIGH,
        preferred_element_type=jnp.float32,
    )


def right_side(slab):
    return jnp.concatenate(
        [jnp.concatenate([slab[0], slab[1]], 1), jnp.concatenate([slab[1], -slab[0]], 1)], 0
    )


def defects(coef, block):
    return jnp.sum(coef[:, None] * (2.0 - block[0] * block[0] - block[1] * block[1]), 0)


def body_plain(matrix_elements, band_index, occupied, band_weight, coulomb):
    bands_dev = matrix_elements.shape[1]
    half = matrix_elements.shape[2]
    n_band = lax.axis_size("band")
    n_bits = n_band.bit_length() - 1
    rows_dev = half // n_band
    n_ga = lax.axis_size("ga")
    chunks = 3 if rows_dev % 3 == 0 else 1
    width = rows_dev // chunks
    factor = 1.0 / math.sqrt(bands_dev * n_band)
    band_pos = lax.axis_index("band")
    ga_pos = lax.axis_index("ga")
    bits = list(range(n_bits - 1))
    top = n_band // 2
    firsts = [b % len(bits) for b in range(chunks)]
    streams = [(c, p) for p in range(2) for c in range(chunks)]
    orders = {}
    for c, p in streams:
        rest = bits[firsts[c] + 1 :] + bits[: firsts[c]]
        orders[c, p] = rest[p:] + rest[:p]

    def swap(x, bit):
        return lax.ppermute(x, "band", [(i, i ^ (1 << bit)) for i in range(n_band)])

    def mine(bit):
        return (band_pos >> bit) & 1

    def pick(x, c, p, which):
        bit = firsts[c]
        parts = []
        for d in range(p * top, (p + 1) * top):
            if not (d >> bit) & 1:
                low = d * rows_dev + c * width
                high = (d | (1 << bit)) * rows_dev + c * width
                parts.append(
                    jnp.where(which == 1, x[..., high : high + width], x[..., low : low + width])
                )
        return jnp.concatenate(parts, -1)

    there = {
        (c, p): swap(pick(matrix_elements, c, p, 1 - mine(firsts[c])), firsts[c])
        for c, p in streams
    }

    occ = (band_index < occupied[0]).astype(jnp.float32)
    coef = (0.5 - occ) * band_weight
    first = matrix_elements[:, :, :COLS]
    moved = lax.ppermute(first, "ga", [(0, g) for g in range(1, n_ga)][:1])
    slab = jnp.where(ga_pos == 0, first, moved)
    scaled = coef[None, :, None] * slab
    right = right_side(scaled)
    rights = [right_side(swap(scaled, bit)) for bit in firsts]
    row_def = defects(coef, matrix_elements)
    col_def = defects(coef, slab)

    sums, left = {}, {}
    for c, p in streams:
        bit = firsts[c]
        rows_here = pick(row_def, c, p, mine(bit))
        send = jnp.concatenate([pick(row_def, c, p, 1 - mine(bit)), col_def])
        got = swap(send, bit)
        count = rows_here.shape[0]
        rows_sum = rows_here + got[:count]
        cols_sum = col_def + got[count:]
        here = pick(matrix_elements, c, p, mine(bit))
        part = contract(here.reshape(2 * bands_dev, count), right)
        part = part + contract(there[c, p].reshape(2 * bands_dev, count), rights[c])
        extra = 0.5 * (rows_sum[:, None] + cols_sum[None, :])
        part = part + jnp.concatenate([extra, jnp.zeros_like(extra)], 1)
        sums[c, p] = part.reshape((2,) * (n_bits - 2) + (width, 2 * COLS))
        left[c, p] = [b for b in reversed(bits) if b != bit]

    for step in range(n_bits - 2):
        sent = {}
        for k in streams:
            bit = orders[k][step]
            send = lax.dynamic_index_in_dim(
                sums[k], 1 - mine(bit), left[k].index(bit), keepdims=False
            )
            sent[k] = swap(send, bit)
        for k in streams:
            bit = orders[k][step]
            keep = lax.dynamic_index_in_dim(sums[k], mine(bit), left[k].index(bit), keepdims=False)
            sums[k] = keep + sent[k]
            left[k].remove(bit)

    upper = mine(n_bits - 1) == 1
    last = [swap(jnp.where(upper, sums[c, 0], sums[c, 1]), n_bits - 1) for c in range(chunks)]
    done = [jnp.where(upper, sums[c, 1], sums[c, 0]) + last[c] for c in range(chunks)]
    total = jnp.concatenate(done, 0)
    row_coul = lax.dynamic_slice_in_dim(coulomb, ga_pos * half + band_pos * rows_dev, rows_dev, 0)
    weight = factor * jnp.sqrt(row_coul[:, None] * coulomb[None, :COLS])
    return jnp.stack([weight * total[:, :COLS], weight * total[:, COLS:]], 1)


def split(value):
    high = value.astype(jnp.bfloat16)
    return high, (value - high.astype(jnp.float32)).astype(jnp.bfloat16)


def kernel(
    rows_dev, factor, m_ref, key_ref, fermi_ref, weight_ref, coul_ref, out_ref,
    keys, weights, coul, rowc, slab, coef, ccol, right, cdef, own, got, left, rdef, part, got2, got3, line,
    small_sem, base_sem, slab_sem, fwd_sem, coef_sem, own_sem, m_sem, s2_sem, s3_sem, line_sem,
):
    bands, half = m_ref.shape[1], m_ref.shape[2]
    width = rows_dev // CHUNKS
    tiles = width // LANES
    me = lax.axis_index("band")
    ga = lax.axis_index("ga")
    mine = [lax.rem(me // (1 << b), 2) for b in range(4)]

    def flip(bit, by):
        return bit + by - 2 * bit * by

    inner = flip(mine[Z_BIT], mine[S_BIT])

    def across(*bits):
        return {"band": me + sum((1 - 2 * mine[b]) * (1 << b) for b in bits)}

    device = {"x": across(X_BIT), "y": across(Y_BIT), "z": across(Z_BIT), "m": across(Z_BIT, S_BIT)}
    sibling = {"ga": 1 - ga}

    def rows_of(c, flips):
        dest = sum(flip(mine[b], flips[b]) * (1 << b) for b in range(4))
        return pl.ds(pl.multiple_of(dest * rows_dev + c * width, LANES), width)

    far_base = 8 * len(LINE) // 2

    def near(c, o, s):
        return c * len(LINE) + LINE.index((o, s))

    def block(*name):
        if len(name) == 4:
            return 2 * near(*name[:3]) + name[3]
        return far_base + 4 * name[1] + name[2]

    def m_rows(sent, *name):
        if len(name) == 4:
            c, o, s, i = name
            first, second = NEAR[c, o, s]
            return rows_of(c, {BIT[first]: sent, BIT[second]: i, Z_BIT: o ^ s, S_BIT: s})
        c, k, i = name
        second, third = FAR[k]
        o, s = (1 - k, 1 - inner) if sent else (k, inner)
        return rows_of(c, {BIT[second]: i // 2, BIT[third]: i % 2, Z_BIT: flip(s, o), S_BIT: s})

    def first_link(name):
        return NEAR[name[:3]][0] if len(name) == 4 else "z"

    def remote(src, dst, sems, k, to):
        return pltpu.make_async_remote_copy(
            src_ref=src, dst_ref=dst, send_sem=sems.at[0, k], recv_sem=sems.at[1, k],
            device_id=to, device_id_type=pl.DeviceIdType.MESH,
        )

    def base_copy():
        return remote(m_ref.at[:, :, pl.ds(0, COLS)], slab.at[0], base_sem, 0, sibling)

    def base_local():
        return pltpu.make_async_copy(m_ref.at[:, :, pl.ds(0, COLS)], slab.at[0], base_sem.at[0, 1])

    def slab_copy(b):
        k = SLOT[b]
        return remote(slab.at[0, ga], slab.at[k, ga], slab_sem, k - 1, device[b])

    def slab_forward(b):
        k = SLOT[b]
        return remote(slab.at[k, ga], slab.at[k, ga], fwd_sem, k - 1, sibling)

    def coef_copy(b):
        k = SLOT[b]
        return remote(coef.at[0], coef.at[k], coef_sem, k - 1, device[b])

    def m_copy(*name):
        k = block(*name)
        return remote(m_ref.at[:, :, m_rows(1, *name)], got.at[k], m_sem, k, device[first_link(name)])

    def own_copy(*name):
        k = block(*name)
        return pltpu.make_async_copy(m_ref.at[:, :, m_rows(0, *name)], own.at[k], own_sem.at[k])

    def s2_of(name):
        if name[0] < 2:
            k = near(*name)
            return NEAR[name][1], k, block(*name, 1), block(*name, 0)
        c, k, r = name
        return FAR[k][0], far_base // 2 + 2 * k + r, block(c, k, 2 + r), block(c, k, r)

    def s2_copy(name):
        link, k, sent, _ = s2_of(name)
        return remote(part.at[sent], got2.at[k], s2_sem, k, device[link])

    def s3_copy(c, k):
        return remote(part.at[block(c, k, 1)], got3.at[k], s3_sem, k, device[FAR[k][1]])

    far_line = 2 * LINE_SLOTS

    def line_copy(src, slot, link):
        return remote(src, line.at[slot], line_sem, slot, device[link])

    def end_slot(c, o, s):
        return c * LINE_SLOTS + LINE_SLOT[o, s]

    def mid_slot(c, o):
        return c * LINE_SLOTS + 3 + o

    small = [
        pltpu.make_async_copy(src, dst, small_sem.at[i])
        for i, (src, dst) in enumerate(((key_ref, keys), (weight_ref, weights), (coul_ref, coul)))
    ]
    barrier = pltpu.get_barrier_semaphore()

    def greet(to):
        pl.semaphore_signal(barrier, inc=1, device_id=to, device_id_type=pl.DeviceIdType.MESH)

    for to in (device["x"], device["y"], device["z"], sibling):
        greet(to)

    @pl.when(inner == 1)
    def _():
        greet(device["m"])

    for copy in small:
        copy.start()

    @pl.when(ga == 0)
    def _():
        base_local().start()

    pl.semaphore_wait(barrier, 4 + inner)

    @pl.when(ga == 0)
    def _():
        base_copy().start()

    def prepare(k):
        column = jnp.broadcast_to(coef[k][0:1, :], (LANES, bands)).T
        ccol[k] = column
        for j in range(COLS // LANES):
            re_at, im_at = pl.ds(j * LANES, LANES), pl.ds(COLS + j * LANES, LANES)
            a, b = slab[k, 0, :, re_at], slab[k, 1, :, re_at]
            total = jnp.sum(column * (2.0 - a * a - b * b), 0, keepdims=True)
            cdef[k, :, re_at] = jnp.broadcast_to(0.5 * total, (8, LANES))
            cdef[k, :, im_at] = jnp.zeros((8, LANES), jnp.float32)
            for level, (sa, sb) in enumerate(zip(split(column * a), split(column * b))):
                right[k, level, :bands, re_at] = sa
                right[k, level, bands:, re_at] = sb
                right[k, level, :bands, im_at] = sb
                right[k, level, bands:, im_at] = -sa

    def prepare_own():
        for copy in small:
            copy.wait()
        occ = (keys[...] < fermi_ref[0]).astype(jnp.float32)
        coef[0] = jnp.broadcast_to((0.5 - occ) * weights[...], coef.shape[1:])
        for t in range(CHUNKS * tiles):
            at = pl.multiple_of(ga * half + me * rows_dev + t * LANES, LANES)
            rowc[t] = jnp.broadcast_to(coul[0:1, pl.ds(at, LANES)], (LANES, LANES)).T

        @pl.when(ga == 0)
        def _():
            base_local().wait()
            base_copy().wait_send()

        @pl.when(ga == 1)
        def _():
            base_copy().wait_recv()

        prepare(0)

    def dots(slot, names):
        for i, name in enumerate(names):
            blk = block(*name)
            own_copy(*name).wait()
            m_copy(*name).wait_recv()
            for t in range(tiles):
                lanes = pl.ds(t * LANES, LANES)
                rows = pl.ds(i * width + t * LANES, LANES)
                total = jnp.zeros((1, LANES), jnp.float32)
                for ref, k, at in ((own, 0, 0), (got, slot, 2 * bands)):
                    a, b = ref[blk, 0, :, lanes], ref[blk, 1, :, lanes]
                    total += jnp.sum(ccol[k] * (2.0 - a * a - b * b), 0, keepdims=True)
                    for level, (sa, sb) in enumerate(zip(split(a.T), split(b.T))):
                        left[level, rows, at : at + bands] = sa
                        left[level, rows, at + bands : at + 2 * bands] = sb
                rdef[rows, :] = jnp.broadcast_to(0.5 * total, (LANES, LANES)).T

        step = 2 * LANES

        def product(n, _):
            at = pl.ds(pl.multiple_of(n * step, step), step)
            acc = None
            for level, other in ((0, 0), (1, 0), (0, 1)):
                for k, k_at in ((0, 0), (slot, 2 * bands)):
                    term = jnp.dot(
                        left[level, :, k_at : k_at + 2 * bands],
                        right[k, other, :, at],
                        preferred_element_type=jnp.float32,
                    )
                    acc = term if acc is None else acc + term
            keep = jnp.where(n * step < COLS, 1.0, 0.0)
            extra = rdef[...] * keep
            acc = acc + jnp.concatenate([extra, extra], 1)
            acc = acc + (cdef[0, 0:1, at] + cdef[slot, 0:1, at])
            for i, name in enumerate(names):
                part[block(*name), :, at] = acc[i * width : (i + 1) * width]
            return 0

        lax.fori_loop(0, 2 * COLS // step, product, 0)

    group = 2 * COLS // LANES

    def finish(c, one, two):
        for t in range(tiles):
            rows = pl.ds(t * LANES, LANES)
            at = pl.ds(c * width + t * LANES, LANES)
            wide = jnp.concatenate([rowc[c * tiles + t]] * (COLS // LANES), 1)
            weight = factor * jnp.sqrt(wide * coul[0:1, :COLS])
            for p in range(2):
                cols = pl.ds(p * COLS, COLS)
                value = weight * (one[rows, cols] + two[rows, cols])
                for j in range(COLS // LANES):
                    spot = (c * width + t * LANES) * group + 2 * j + p
                    out_ref[pl.ds(spot, LANES, stride=group), :] = value[:, j * LANES : (j + 1) * LANES]

    flying = {}

    def only(cls, action):
        if cls == "B":
            action()
        else:
            pl.when(inner == (1 if cls == "I" else 0))(action)

    def wait_sent(copies):
        for make in copies:
            make().wait_send()

    def send(cls, link, *copies):
        entry = list(copies)
        waits = {}
        for c in "OI" if cls == "B" else cls:
            queue = flying.setdefault((c, link), [])
            if len(queue) >= DEPTH:
                waits[c] = queue.pop(0)
            queue.append(entry)
        if len(waits) == 2 and waits["O"] is waits["I"]:
            wait_sent(waits["O"])
            waits = {}
        for c, copies in waits.items():
            only(c, functools.partial(wait_sent, copies))

        def start():
            for make in entry:
                make().start()

        only(cls, start)

    def add(cls, copy, blk, ref, k):
        def action():
            copy().wait_recv()
            part[blk] += ref[k]

        only(cls, action)

    def do(f, *args):
        return functools.partial(f, *args)

    loads = [e[1:] for e in STEPS if e[0] == "m"]
    for e in STEPS:
        kind, rest = e[0], e[1:]
        if kind == "prep" and rest[0] == "o":
            for name in loads:
                own_copy(*name).start()
            prepare_own()
        elif kind == "slab":
            send("B", rest[0], do(slab_copy, *rest), do(coef_copy, *rest))
        elif kind == "fwd":
            slab_copy(*rest).wait_recv()
            slab_forward(*rest).start()
        elif kind == "prep":
            slab_forward(*rest).wait()
            coef_copy(*rest).wait_recv()
            prepare(SLOT[rest[0]])
        elif kind == "m":
            send("B", first_link(rest), do(m_copy, *rest))
        elif kind == "dot" and len(rest) == 3 and rest[0] < 2:
            dots(SLOT[NEAR[rest][0]], [rest + (i,) for i in range(2)])
        elif kind == "dot":
            c, k, j = rest
            dots(SLOT["z"], [(c, k, 2 * j + i) for i in range(2)])
        elif kind == "s2":
            send("B", s2_of(rest)[0], do(s2_copy, rest))
        elif kind == "a2":
            _, k, _, blk = s2_of(rest)
            add("B", do(s2_copy, rest), blk, got2, k)
        elif kind == "s3":
            send("B", FAR[rest[1]][1], do(s3_copy, *rest))
        elif kind == "a3":
            add("B", do(s3_copy, *rest), block(*rest, 0), got3, rest[1])
        elif kind == "osend":
            c, o, s = rest
            slot = end_slot(c, 1 - o, s)
            send("O", "z", do(line_copy, part.at[block(*rest, 0)], slot, "z"))
        elif kind == "iadd":
            slot = end_slot(*rest)
            add("I", do(line_copy, line.at[slot], slot, "z"), block(*rest, 0), line, slot)
        elif kind == "imid":
            c, o, s = rest
            send("I", "m", do(line_copy, part.at[block(*rest, 0)], mid_slot(c, o), "m"))
        elif kind == "imadd":
            slot = mid_slot(rest[0], 1)
            add("I", do(line_copy, line.at[slot], slot, "m"), block(*rest, 0), line, slot)
        elif kind == "iout":
            (c,) = rest
            send("I", "z", do(line_copy, part.at[block(c, 1, 0, 0)], c * LINE_SLOTS, "z"))
        elif kind in ("ifin", "ofin"):
            (c,) = rest
            slot, link = (mid_slot(c, 0), "m") if kind == "ifin" else (c * LINE_SLOTS, "z")

            def action(c=c, slot=slot, link=link):
                line_copy(line.at[slot], slot, link).wait_recv()
                finish(c, part.at[block(c, 0, 0, 0)], line.at[slot])

            only("I" if kind == "ifin" else "O", action)
        elif kind == "imid2":
            (k,) = rest
            send("I", "m", do(line_copy, part.at[block(2, k, 0)], far_line + 1 + k, "m"))
        elif kind == "osend2":
            send("O", "z", do(line_copy, part.at[block(2, 1, 0)], far_line, "z"))
        elif kind == "iout2":
            def arrived():
                line_copy(line.at[far_line + 2], far_line + 2, "m").wait_recv()

            only("I", arrived)
            send("I", "z", do(line_copy, line.at[far_line + 2], far_line, "z"))
        elif kind == "ifin2":
            def action():
                line_copy(line.at[far_line + 1], far_line + 1, "m").wait_recv()
                line_copy(line.at[far_line], far_line, "z").wait_recv()
                finish(2, line.at[far_line], line.at[far_line + 1])

            only("I", action)
        elif kind == "ofin2":
            def action():
                line_copy(line.at[far_line], far_line, "z").wait_recv()
                finish(2, part.at[block(2, 0, 0)], line.at[far_line])

            only("O", action)

    for c in "OI":
        def drain(c=c):
            for (cls, _), queue in flying.items():
                for copies in queue if cls == c else ():
                    wait_sent(copies)

        only(c, drain)


def body_fast(matrix_elements, band_index, occupied, band_weight, coulomb):
    bands = matrix_elements.shape[1]
    half = matrix_elements.shape[2]
    n_band = lax.axis_size("band")
    rows_dev = half // n_band
    width = rows_dev // CHUNKS
    factor = 1.0 / math.sqrt(bands * n_band)
    f32 = jnp.float32
    hbm = pl.BlockSpec(memory_space=pl.ANY)
    blocks = 8 * CHUNKS
    near_streams = 2 * len(LINE)
    dma = pltpu.SemaphoreType.DMA
    total = pl.pallas_call(
        functools.partial(kernel, rows_dev, factor),
        out_shape=pltpu.VMEM((rows_dev * 2 * COLS // LANES, LANES), f32),
        in_specs=[hbm, hbm, pl.BlockSpec(memory_space=pltpu.SMEM), hbm, hbm],
        out_specs=pl.BlockSpec(memory_space=pltpu.VMEM),
        scratch_shapes=[
            pltpu.VMEM((1, bands), jnp.int32),
            pltpu.VMEM((1, bands), f32),
            pltpu.VMEM((1, coulomb.shape[0]), f32),
            pltpu.VMEM((rows_dev // LANES, LANES, LANES), f32),
            pltpu.VMEM((4, 2, bands, COLS), f32),
            pltpu.VMEM((4, 8, bands), f32),
            pltpu.VMEM((4, bands, LANES), f32),
            pltpu.VMEM((4, 2, 2 * bands, 2 * COLS), jnp.bfloat16),
            pltpu.VMEM((4, 8, 2 * COLS), f32),
            pltpu.VMEM((blocks, 2, bands, width), f32),
            pltpu.VMEM((blocks, 2, bands, width), f32),
            pltpu.VMEM((2, 2 * width, 4 * bands), jnp.bfloat16),
            pltpu.VMEM((2 * width, LANES), f32),
            pltpu.VMEM((blocks, width, 2 * COLS), f32),
            pltpu.VMEM((near_streams + 4, width, 2 * COLS), f32),
            pltpu.VMEM((2, width, 2 * COLS), f32),
            pltpu.VMEM((2 * LINE_SLOTS + 3, width, 2 * COLS), f32),
            dma((3,)), dma((2, 2)), dma((2, 3)), dma((2, 3)), dma((2, 3)), dma((blocks,)),
            dma((2, blocks)), dma((2, near_streams + 4)), dma((2, 2)), dma((2, 2 * LINE_SLOTS + 3)),
        ],
        compiler_params=pltpu.CompilerParams(
            collective_id=0, has_side_effects=True, vmem_limit_bytes=VMEM_BYTES
        ),
        name="reduce_sums",
    )(
        matrix_elements, band_index.reshape(1, bands), occupied, band_weight.reshape(1, bands),
        coulomb.reshape(1, coulomb.shape[0]),
    )
    parts = total.reshape(rows_dev, COLS // LANES, 2, LANES)
    return parts.transpose(0, 2, 1, 3).reshape(rows_dev, 2, COLS)


def solution(mesh):
    n_band, n_ga = mesh.shape["band"], mesh.shape["ga"]

    def body(matrix_elements, *rest):
        rows_dev = matrix_elements.shape[2] // n_band
        aligned = rows_dev % (CHUNKS * LANES) == 0 and matrix_elements.shape[1] % LANES == 0
        if n_band == 1 << len(LINE) and n_ga == 2 and aligned:
            return body_fast(matrix_elements, *rest)
        return body_plain(matrix_elements, *rest)

    return jax.shard_map(
        body,
        mesh=mesh,
        in_specs=(P(None, "band", "ga"), P("band"), P(), P("band"), P()),
        out_specs=P(("ga", "band"), None, None),
        check_vma=False,
    )
```
